32 devices in a mesh: space: 16 (over z, x, core), vel: 2 (over y).
Axes of the slice: x: 2, y: 2, z: 4, core: 2. Of those that a mesh axis runs over, the one named last changes fastest.
Arguments:
- dist: float32 [64, 8, 8, 4096], P('space', None, None, 'vel'), may hold values from 0 to 5.5, as said below
- cell_type: int32 [64, 8, 8], replicated, may hold values from 0 to 3, as said below
- boundary: float32 [6], replicated, may hold values from 0.8 to 1.2
Outputs:
- renewed: float32 [64, 8, 8, 4096], P('space', None, None, 'vel')
The draws below stay inside these ranges and needn't reach their ends.
Inputs may be any that keep to these rules, and one draw needn't show every extreme that they name: `dist`: every entry is positive. `cell_type`: cells of kind 1 never lie on the grid's outer layer; kind 2 lies only in the plane x = 0 and kind 3 only in the plane x = 63, and both occur in every draw.
All inputs are finite; a program needn't handle non-finite values.
Results may differ from the reference program's by a relative error of at most 0.0003.
Values sent between devices are 32-bit elements; how exact they have to be, the bound alone decides.
No kernel may reach another device: no remote copies, remote signals or barrier semaphores. Data moves between devices by JAX's collectives and lax.ppermute only.
A program may use at most 64 MiB of HBM per device.

```python
import math
import jax
import jax.numpy as jnp
from jax import lax

NODES = 16
VELOCITIES = 4096
CELLS_Y = 8
CELLS_Z = 8
STEPS = 2
CELLS_X = 64


VMAX = 5.0


def draw_dist(key, part):
    keys = jax.random.split(jax.random.fold_in(key, 101), 10)
    shape = (CELLS_X, CELLS_Y, CELLS_Z)
    density = jnp.exp(jax.random.uniform(keys[0], shape, jnp.float32, math.log(0.5), math.log(2.0)))
    stream = jax.random.uniform(keys[1], shape, jnp.float32, 0.2, 1.2)
    noise = 0.08 * jax.random.truncated_normal(keys[5], -3.0, 3.0, shape + (VELOCITIES,), jnp.float32)
    drift_y = jax.random.uniform(keys[2], shape, jnp.float32, -0.3, 0.3)
    drift_z = jax.random.uniform(keys[3], shape, jnp.float32, -0.3, 0.3)
    temper = jax.random.uniform(keys[4], shape, jnp.float32, 0.7, 1.4)
    second_temper = jax.random.uniform(keys[6], shape, jnp.float32, 0.7, 1.4)
    share = jax.random.uniform(keys[7], shape, jnp.float32, 0.1, 0.4)
    jump = jax.random.uniform(keys[8], shape + (3,), jnp.float32, -1.0, 1.0)
    number = jnp.arange(VELOCITIES, dtype=jnp.int32)
    spacing = 2.0 * VMAX / NODES
    along_x = ((number // (NODES * NODES)).astype(jnp.float32) + 0.5) * spacing - VMAX
    along_y = ((number // NODES % NODES).astype(jnp.float32) + 0.5) * spacing - VMAX
    along_z = ((number % NODES).astype(jnp.float32) + 0.5) * spacing - VMAX

    def maxwell(center_x, center_y, center_z, heat_level):
        square = (along_x - center_x[..., None]) ** 2 + (along_y - center_y[..., None]) ** 2 + (along_z - center_z[..., None]) ** 2
        amplitude = density / (heat_level * jnp.sqrt(heat_level))
        return amplitude[..., None] * jnp.exp(-square / (2.0 * heat_level[..., None]))
    first_part = maxwell(stream, drift_y, drift_z, temper)
    second_part = maxwell(stream + jump[..., 0], drift_y + jump[..., 1], drift_z + jump[..., 2], second_temper)
    mixed = (1.0 - share[..., None]) * first_part + share[..., None] * second_part
    return mixed * (1.0 + noise)


def draw_cell_type(key, part):
    keys = jax.random.split(jax.random.fold_in(key, 202), 3)
    radius_y = jax.random.randint(keys[0], (CELLS_X,), max(CELLS_Y // 4, 1), max(CELLS_Y // 2, 2))
    radius_z = jax.random.randint(keys[1], (CELLS_X,), max(CELLS_Z // 4, 1), max(CELLS_Z // 2, 2))
    plane = jnp.arange(CELLS_X, dtype=jnp.int32)[:, None, None]
    across = jnp.arange(CELLS_Y, dtype=jnp.int32)[None, :, None]
    height = jnp.arange(CELLS_Z, dtype=jnp.int32)[None, None, :]
    open_y = jnp.abs(2 * across - (CELLS_Y - 1)) < 2 * radius_y[:, None, None]
    open_z = jnp.abs(2 * height - (CELLS_Z - 1)) < 2 * radius_z[:, None, None]
    opening = open_y & open_z
    interior = (plane > 0) & (plane < CELLS_X - 1)
    obstacle = (jax.random.randint(keys[2], (CELLS_X, CELLS_Y, CELLS_Z), 0, 6) == 0) & interior
    kinds = jnp.where(opening & jnp.logical_not(obstacle), 1, 0)
    kinds = jnp.where(opening & (plane == 0), 2, kinds)
    kinds = jnp.where(opening & (plane == CELLS_X - 1), 3, kinds)
    return kinds.astype(jnp.int32)


def setup_inputs(seed: int = 0) -> dict:
    key_of = jax.random.split(jax.random.key(seed), 4)
    dist = draw_dist(jax.random.fold_in(key_of[3], 71), 0)
    cell_type = draw_cell_type(jax.random.fold_in(key_of[3], 71), 0)
    boundary = jnp.clip(jax.random.uniform(key_of[2], (6,), jnp.float32, 0.8, 1.2), 0.8, 1.2)
    return {"dist": dist, "cell_type": cell_type, "boundary": boundary}


PRANDTL = 2.0 / 3.0
OMEGA = 0.81
MU_REF = 0.1
DT = 0.1
HALF = 0.05
VMAX = 5.0
PRECISE = lax.Precision.HIGHEST

def speeds_of(start, count):
    number = start + jnp.arange(count, dtype=jnp.int32)
    spacing = 2.0 * VMAX / NODES
    digits = (number // (NODES * NODES), number // NODES % NODES, number % NODES)
    return tuple(((node_digit.astype(jnp.float32) + 0.5) * spacing - VMAX for node_digit in digits))

def node_weight():
    return (2.0 * VMAX / NODES) ** 3 / (2.0 * math.pi) ** 1.5

def offsets(velocity, speeds):
    shifted = tuple((speeds[component] - velocity[component][..., None] for component in range(3)))
    square = shifted[0] * shifted[0] + shifted[1] * shifted[1] + shifted[2] * shifted[2]
    return (shifted, square)

def maxwellian(density, velocity, temper, speeds):
    shifted, square = offsets(velocity, speeds)
    amplitude = density / (temper * jnp.sqrt(temper))
    return amplitude[..., None] * jnp.exp(-square / (2.0 * temper[..., None]))

def shakhov(density, velocity, temper, heat_flux, speeds):
    shifted, square = offsets(velocity, speeds)
    amplitude = density / (temper * jnp.sqrt(temper))
    maxwell_part = amplitude[..., None] * jnp.exp(-square / (2.0 * temper[..., None]))
    projected = shifted[0] * heat_flux[0][..., None] + shifted[1] * heat_flux[1][..., None] + shifted[2] * heat_flux[2][..., None]
    factor = (1.0 - PRANDTL) / (5.0 * density * temper * temper)
    return maxwell_part * (1.0 + factor[..., None] * projected * (square / temper[..., None] - 5.0))

def relaxation(density, temper):
    return MU_REF * jnp.exp(OMEGA * jnp.log(temper)) / (density * temper)

def plain_table(speeds, weight):
    square = speeds[0] * speeds[0] + speeds[1] * speeds[1] + speeds[2] * speeds[2]
    return weight * jnp.stack([jnp.ones_like(square), speeds[0], speeds[1], speeds[2], 0.5 * square])

def project(values, moment_table):
    return jnp.einsum('pyzv,mv->mpyz', values, moment_table, precision=PRECISE)

def primitives(totals):
    density = totals[0]
    velocity = tuple((totals[1 + component] / density for component in range(3)))
    speed_sq = velocity[0] * velocity[0] + velocity[1] * velocity[1] + velocity[2] * velocity[2]
    temper = (2.0 * totals[4] / density - speed_sq) / 3.0
    return (density, velocity, temper)

def heat_terms(values, velocity, speeds, weight):
    shifted, square = offsets(velocity, speeds)
    energy = 0.5 * weight * square * values
    return jnp.stack([lax.optimization_barrier(jnp.sum(shifted[component] * energy, axis=-1)) for component in range(3)])

def limited(ahead, behind):
    return 0.5 * (jnp.sign(ahead) + jnp.sign(behind)) * jnp.minimum(jnp.abs(ahead), jnp.abs(behind))

def reconstruct(values, kinds, speeds, cell, ghost):
    density, velocity, temper, heat_flux, tau = cell
    target = shakhov(density, velocity, temper, heat_flux, speeds)
    spread = 2.0 * tau[..., None]
    before = ((spread - HALF) * values + 3.0 * HALF * target) / (spread + DT)
    middle = before[1:-1]
    planes, across, height, nodes_here = middle.shape
    side_y = jnp.broadcast_to(ghost, (planes, 1, height, nodes_here))
    padded = jnp.concatenate([side_y, middle, side_y], axis=1)
    slope_y = limited(padded[:, 2:] - middle, middle - padded[:, :-2])
    side_z = jnp.broadcast_to(ghost, (planes, across, 1, nodes_here))
    padded = jnp.concatenate([side_z, middle, side_z], axis=2)
    slope_z = limited(padded[:, :, 2:] - middle, middle - padded[:, :, :-2])
    slope_x = limited(before[2:] - middle, middle - before[:-2])
    fluid = (kinds[1:-1] == 1)[..., None]
    slope_x = jnp.where(fluid, slope_x, 0.0)
    slope_y = jnp.where(fluid, slope_y, 0.0)
    slope_z = jnp.where(fluid, slope_z, 0.0)
    centre = middle - HALF * (speeds[0] * slope_x + speeds[1] * slope_y + speeds[2] * slope_z)
    face_x = jnp.where(speeds[0] > 0, (centre + 0.5 * slope_x)[:-1], (centre - 0.5 * slope_x)[1:])
    inner = centre[1:-1]
    upper_y = inner + 0.5 * slope_y[1:-1]
    lower_y = inner - 0.5 * slope_y[1:-1]
    side_y = jnp.broadcast_to(ghost, (planes - 2, 1, height, nodes_here))
    face_y = jnp.where(speeds[1] > 0, jnp.concatenate([side_y, upper_y], axis=1), jnp.concatenate([lower_y, side_y], axis=1))
    upper_z = inner + 0.5 * slope_z[1:-1]
    lower_z = inner - 0.5 * slope_z[1:-1]
    side_z = jnp.broadcast_to(ghost, (planes - 2, across, 1, nodes_here))
    face_z = jnp.where(speeds[2] > 0, jnp.concatenate([side_z, upper_z], axis=2), jnp.concatenate([lower_z, side_z], axis=2))
    return (before, (face_x, face_y, face_z))

def face_flux(face, state, speeds):
    density, velocity, temper, heat_flux = state
    tau = relaxation(density, temper)
    heat_flux = tuple((2.0 * tau * component / (2.0 * tau + HALF * PRANDTL) for component in heat_flux))
    target = shakhov(density, velocity, temper, heat_flux, speeds)
    spread = 2.0 * tau[..., None]
    return (spread * face + HALF * target) / (spread + HALF)

def renew(values, before, fluxes, kinds, speeds, cell, boundary):
    density = cell[0][2:-2]
    velocity = tuple((component[2:-2] for component in cell[1]))
    plus = (4.0 * before[2:-2] - values[2:-2]) / 3.0
    flux_x, flux_y, flux_z = fluxes
    change = speeds[0] * (flux_x[1:] - flux_x[:-1]) + speeds[1] * (flux_y[:, 1:] - flux_y[:, :-1]) + speeds[2] * (flux_z[:, :, 1:] - flux_z[:, :, :-1])
    fresh = plus - DT * change
    blank = jnp.zeros_like(density)
    inlet = maxwellian(boundary[0] + blank, (boundary[1] + blank, blank, blank), boundary[2] + blank, speeds)
    outlet = maxwellian(boundary[3] + blank, velocity, boundary[4] + blank, speeds)
    wall = maxwellian(density, (blank, blank, blank), boundary[5] + blank, speeds)
    kind = kinds[2:-2][..., None]
    return jnp.where(kind == 1, fresh, jnp.where(kind == 2, inlet, jnp.where(kind == 3, outlet, wall)))

def step(values, kinds, boundary):
    block = min(VELOCITIES, 512)
    count = VELOCITIES // block
    weight = node_weight()
    blank = jnp.zeros((), jnp.float32)
    ghost_all = maxwellian(boundary[3], (blank, blank, blank), boundary[5], speeds_of(0, VELOCITIES))
    ghost_planes = jnp.broadcast_to(ghost_all, (2, CELLS_Y, CELLS_Z, VELOCITIES))
    padded = jnp.concatenate([ghost_planes, values, ghost_planes], axis=0)
    kinds_pad = jnp.pad(kinds, ((2, 2), (0, 0), (0, 0)))
    numbers = jnp.arange(count, dtype=jnp.int32)

    def piece(number):
        start = number * block
        return (lax.dynamic_slice_in_dim(padded, start, block, 3), speeds_of(start, block))

    def cell_sum(number):
        portion, nodes = piece(number)
        return project(portion, plain_table(nodes, weight))
    density, velocity, temper = primitives(lax.optimization_barrier(jnp.sum(lax.map(cell_sum, numbers), axis=0)))

    def cell_heat(number):
        portion, nodes = piece(number)
        return heat_terms(portion, velocity, nodes, weight)
    heat_sum = lax.optimization_barrier(jnp.sum(lax.map(cell_heat, numbers), axis=0))
    tau = relaxation(density, temper)
    heat_flux = tuple((heat_sum[component] / (1.0 + DT * PRANDTL / (2.0 * tau)) for component in range(3)))
    cell = (density, velocity, temper, heat_flux, tau)

    def faces_of(number):
        portion, nodes = piece(number)
        ghost = lax.dynamic_slice_in_dim(ghost_all, number * block, block, 0)
        return (nodes, portion, reconstruct(portion, kinds_pad, nodes, cell, ghost))

    def face_sum(number):
        nodes, portion, rebuilt = faces_of(number)
        moment_table = plain_table(nodes, weight)
        return tuple((project(face, moment_table) for face in rebuilt[1]))
    states = [primitives(lax.optimization_barrier(jnp.sum(member, axis=0))) for member in lax.map(face_sum, numbers)]

    def face_heat(number):
        nodes, portion, rebuilt = faces_of(number)
        return tuple((heat_terms(face, state[1], nodes, weight) for face, state in zip(rebuilt[1], states)))
    flux_sums = [lax.optimization_barrier(jnp.sum(member, axis=0)) for member in lax.map(face_heat, numbers)]
    states = [state + ((flux_sum[0], flux_sum[1], flux_sum[2]),) for state, flux_sum in zip(states, flux_sums)]

    def renewed_block(number):
        nodes, portion, rebuilt = faces_of(number)
        fluxes = [face_flux(face, state, nodes) for face, state in zip(rebuilt[1], states)]
        return renew(portion, rebuilt[0], fluxes, kinds_pad, nodes, cell, boundary)
    blocks = lax.map(renewed_block, numbers)
    return jnp.moveaxis(blocks, 0, 3).reshape(CELLS_X, CELLS_Y, CELLS_Z, VELOCITIES)

def reference(dist, cell_type, boundary):
    values = dist
    for turn in range(STEPS):
        values = step(values, cell_type, boundary)
    return values
```

```python
import functools
import math

import jax
import jax.numpy as jnp
import numpy as np
from jax import lax
from jax.experimental import pallas as pl
from jax.experimental.pallas import tpu as pltpu
from jax.sharding import PartitionSpec as P

NODES = 16
STEPS = 2
PRANDTL = 2.0 / 3.0
OMEGA = 0.81
MU_REF = 0.1
DT = 0.1
HALF = 0.05
VMAX = 5.0
SPACING = 2.0 * VMAX / NODES
UNIT = 0.5 * SPACING
WEIGHT = SPACING**3 / (2.0 * math.pi) ** 1.5
LOG2E = 1.4426950408889634
COLS = 16
TILE = NODES * NODES
ROWS = 8
HALFTILE = 128


def node_table():
    number = np.arange(NODES**3)
    digits = (number // (NODES * NODES), number // NODES % NODES, number % NODES)
    m = [2 * d + 1 - NODES for d in digits]
    n = m[0] * m[0] + m[1] * m[1] + m[2] * m[2]
    third = [c * n for c in m]
    high = [((v + 32) // 64) * 64 for v in third]
    low = [v - h for v, h in zip(third, high)]
    base = [np.ones_like(n), *m, m[0] * m[0], m[1] * m[1], m[2] * m[2]]
    base += [m[0] * m[1], m[0] * m[2], m[1] * m[2], *high, *low]
    table = np.zeros((HALFTILE, NODES**3), np.float32)
    for part in range(3):
        table[part * COLS : (part + 1) * COLS] = np.stack(base)
    return jnp.asarray(table, jnp.bfloat16)


def dot_nt(a, b):
    return lax.dot_general(a, b, (((1,), (1,)), ((), ())), preferred_element_type=jnp.float32)


def dot_nn(a, b):
    return lax.dot_general(a, b, (((1,), (0,)), ((), ())), preferred_element_type=jnp.float32)


def split(value):
    high = value.astype(jnp.bfloat16)
    low = (value - high.astype(jnp.float32)).astype(jnp.bfloat16)
    return high, low


def state_of(t):
    density = t[0]
    second_unit = UNIT * UNIT
    velocity = [UNIT * t[1 + e] / density for e in range(3)]
    second = (
        (second_unit * t[4], second_unit * t[7], second_unit * t[8]),
        (second_unit * t[7], second_unit * t[5], second_unit * t[9]),
        (second_unit * t[8], second_unit * t[9], second_unit * t[6]),
    )
    trace = second[0][0] + second[1][1] + second[2][2]
    speed_sq = velocity[0] * velocity[0] + velocity[1] * velocity[1] + velocity[2] * velocity[2]
    temper = (trace / density - speed_sq) / 3.0
    heat = [
        0.5
        * (
            (UNIT**3) * (t[10 + e] + t[13 + e])
            - 2.0
            * (
                second[e][0] * velocity[0]
                + second[e][1] * velocity[1]
                + second[e][2] * velocity[2]
            )
            - velocity[e] * trace
            + 2.0 * density * velocity[e] * speed_sq
        )
        for e in range(3)
    ]
    return density, velocity, temper, heat


def relaxation(density, temper):
    return MU_REF * jnp.exp(OMEGA * jnp.log(temper)) / (density * temper)


def exponent_coefs(velocity, temper):
    g = -0.5 * LOG2E / temper
    speed_sq = velocity[0] * velocity[0] + velocity[1] * velocity[1] + velocity[2] * velocity[2]
    square = g * (UNIT * UNIT)
    zero = jnp.zeros_like(g)
    linear = [(-2.0 * UNIT) * g * velocity[e] for e in range(3)]
    return [g * speed_sq, *linear, square, square, square] + [zero] * 9


def shakhov_coefs(amplitude, density, velocity, temper, heat):
    factor = (1.0 - PRANDTL) / (5.0 * density * temper * temper)
    af = amplitude * factor
    inverse = 1.0 / temper
    along = velocity[0] * heat[0] + velocity[1] * heat[1] + velocity[2] * heat[2]
    speed_sq = velocity[0] * velocity[0] + velocity[1] * velocity[1] + velocity[2] * velocity[2]
    a2 = (UNIT * UNIT) * inverse
    b = [(-2.0 * UNIT) * velocity[e] * inverse for e in range(3)]
    c = speed_sq * inverse - 5.0
    kq = [UNIT * heat[e] for e in range(3)]
    cubic = [af * (kq[e] * a2) for e in range(3)]
    return [
        amplitude - af * (along * c),
        *[af * (kq[e] * c - along * b[e]) for e in range(3)],
        *[af * (kq[e] * b[e] - along * a2) for e in range(3)],
        af * (kq[0] * b[1] + kq[1] * b[0]),
        af * (kq[0] * b[2] + kq[2] * b[0]),
        af * (kq[1] * b[2] + kq[2] * b[1]),
        *cubic,
        *cubic,
    ]


def transposed_parts(coefs, extra, work):
    count = work.shape[1]
    work[...] = jnp.zeros(work.shape, jnp.float32)
    for row, value in enumerate(coefs):
        high = value.astype(jnp.bfloat16).astype(jnp.float32)
        rest = value - high
        middle = rest.astype(jnp.bfloat16).astype(jnp.float32)
        work[row : row + 1, :] = high
        work[COLS + row : COLS + row + 1, :] = middle
        work[2 * COLS + row : 2 * COLS + row + 1, :] = rest - middle
    if extra is not None:
        work[3 * COLS : 3 * COLS + 1, :] = extra
    return jnp.transpose(work[...], (1, 0))


def spread_column(matrix):
    return jnp.broadcast_to(matrix[:, 3 * COLS : 3 * COLS + 1], (matrix.shape[0], HALFTILE))


def twice(value):
    return jnp.concatenate([value, value], axis=1)


def lane_speeds(shape):
    lane = lax.broadcasted_iota(jnp.int32, shape, 1)
    along_y = (2 * (lane // NODES) + 1 - NODES).astype(jnp.float32) * UNIT
    along_z = (2 * (lane % NODES) + 1 - NODES).astype(jnp.float32) * UNIT
    return along_y, along_z


def moments_kernel(x_ref, table_ref, out_ref, acc_ref):
    n = pl.program_id(0)

    @pl.when(n == 0)
    def _():
        acc_ref[...] = jnp.zeros_like(acc_ref)

    high, low = split(x_ref[...])
    acc_ref[...] += dot_nt(high, table_ref[...]) + dot_nt(low, table_ref[...])

    @pl.when(n == pl.num_programs(0) - 1)
    def _():
        out_ref[...] = WEIGHT * jnp.transpose(acc_ref[...], (1, 0))[:COLS]


def faces_kernel(
    scal_ref, x_ref, upw_ref, dn_ref, tot_ref, mask_ref, table_ref,
    base_ref, face_ref, mom_ref,
    work_ref, full_ref, lhs_ref, alpha_ref, res_ref, slab_ref, high_ref, low_ref, acc_ref,
    *, planes,
):
    n = pl.program_id(0)
    neg = scal_ref[0]
    cells = ROWS * ROWS
    slots = planes + 3
    slab_rows = slots * cells
    inner = (ROWS - 2) * ROWS
    face_y = (planes + 1) * inner
    face_z = face_y + planes * cells
    faces = face_z + planes * inner

    @pl.when(n == 0)
    def _():
        t = [tot_ref[i : i + 1, :] for i in range(COLS)]
        density, velocity, temper, heat = state_of(t)
        tau = relaxation(density, temper)
        heat = [q / (1.0 + DT * PRANDTL / (2.0 * tau)) for q in heat]
        divide = 1.0 / (2.0 * tau + DT)
        alpha = (2.0 * tau - HALF) * divide
        beta = (3.0 * HALF) * divide
        amplitude = beta * (density / (temper * jnp.sqrt(temper)))
        turned = transposed_parts(exponent_coefs(velocity, temper), alpha, work_ref)
        full_ref[...] = turned
        first = pl.multiple_of(neg * cells, cells)
        part = full_ref[pl.ds(first, slab_rows), :]
        lhs_ref[0:slab_rows, :] = part.astype(jnp.bfloat16)
        alpha_ref[...] = spread_column(part)
        turned = transposed_parts(
            shakhov_coefs(amplitude, density, velocity, temper, heat), None, work_ref
        )
        full_ref[...] = turned
        part = full_ref[pl.ds(first, slab_rows), :]
        lhs_ref[slab_rows : 2 * slab_rows, :] = part.astype(jnp.bfloat16)
        acc_ref[...] = jnp.zeros_like(acc_ref)

    table = table_ref[...]
    res_ref[...] = dot_nn(lhs_ref[...], table)

    def before_of(src_ref, row, slot, base_row=None):
        for r in range(0, cells, 16):
            f = src_ref[row + r : row + r + 16, :]
            at = pl.multiple_of(slot * cells + r, 16)
            exponent = res_ref[pl.ds(at, 16), :]
            poly = res_ref[pl.ds(pl.multiple_of(at + slab_rows, 16), 16), :]
            b = twice(alpha_ref[pl.ds(at, 16), :]) * f + jnp.exp2(exponent) * poly
            slab_ref[slot, r : r + 16, :] = b
            if base_row is not None:
                base_ref[base_row + r : base_row + r + 16, :] = (4.0 / 3.0) * b - (1.0 / 3.0) * f

    for p in range(planes):
        before_of(x_ref, p * cells, p + 2 - neg, p * cells)
    before_of(upw_ref, 0, (planes + 1) * neg)
    before_of(upw_ref, cells, (planes + 1) * neg + 1)
    before_of(dn_ref, 0, (planes + 2) * (1 - neg))

    along_y, along_z = lane_speeds((ROWS, TILE))
    lane = lax.broadcasted_iota(jnp.int32, (ROWS, TILE), 1)
    z_minus = (lane % NODES) < NODES // 2
    ky = HALF * along_y
    kz = HALF * along_z
    hy = jnp.where(lane < HALFTILE, -0.5, 0.5)
    hz = jnp.where(z_minus, -0.5, 0.5)
    digit = scal_ref[1] + n
    along_x = (2 * digit + 1 - NODES).astype(jnp.float32) * UNIT
    kx = HALF * along_x
    hx = jnp.where(along_x > 0, 0.5, -0.5)

    def middle(a, b):
        return jnp.maximum(jnp.minimum(a, b), jnp.minimum(jnp.maximum(a, b), 0.0))

    def put(row, pair):
        both = jnp.concatenate(pair, axis=0)
        high, low = split(both)
        at = pl.ds(pl.multiple_of(row, 16), 16)
        face_ref[at, :] = both
        high_ref[at, :] = high
        low_ref[at, :] = low

    def plane_faces(slot, own):
        def col(y):
            return slab_ref[slot, y * ROWS : (y + 1) * ROWS, :]

        values = {0: col(0), 1: col(1)}
        diff = values[1] - values[0]
        fx, fy, fz = {}, {0: values[0], ROWS - 1: col(ROWS - 1)}, {}
        for y in range(1, ROWS - 1):
            here = values[y]
            values[y + 1] = col(y + 1)
            back, diff = diff, values[y + 1] - here
            rows = slice(y * ROWS, (y + 1) * ROWS)
            mask = twice(mask_ref[pl.ds(pl.multiple_of(slot * cells + y * ROWS, ROWS), ROWS), :])
            slope_y = middle(diff, back) * mask
            slope_x = mask * middle(
                slab_ref[slot + 1, rows, :] - here, here - slab_ref[slot - 1, rows, :]
            )
            step = here - pltpu.roll(here, 1, 0)
            slope_z = middle(pltpu.roll(step, ROWS - 1, 0), step) * mask
            centre = here - (kx * slope_x + ky * slope_y + kz * slope_z)
            fx[y] = centre + hx * slope_x
            if own is not None:
                fy[y] = centre + hy * slope_y
                side = centre + hz * slope_z
                fz[y] = jnp.where(z_minus, side, pltpu.roll(side, 1, 0))
        for i in range((ROWS - 2) // 2):
            row = (slot - 1) * inner + 16 * i
            put(row, [fx[1 + 2 * i], fx[2 + 2 * i]])
        if own is not None:
            gy = [fy[0]]
            for j in range(1, ROWS):
                gy.append(jnp.concatenate([fy[j][:, :HALFTILE], fy[j - 1][:, HALFTILE:]], axis=1))
            for i in range(ROWS // 2):
                put(face_y + own * cells + 16 * i, [gy[2 * i], gy[2 * i + 1]])
            for i in range((ROWS - 2) // 2):
                put(face_z + own * inner + 16 * i, [fz[1 + 2 * i], fz[2 + 2 * i]])

    for slot in range(2, planes + 1):
        plane_faces(slot, slot - 2 + neg)
    edge = (planes + 1) - planes * neg
    plane_faces(edge, edge - 2 + neg)
    plane_faces(1 + planes * neg, None)

    acc_ref[0:faces, :] += dot_nt(high_ref[...], table) + dot_nt(low_ref[...], table)

    @pl.when(n == pl.num_programs(0) - 1)
    def _():
        mom_ref[...] = WEIGHT * jnp.transpose(acc_ref[...], (1, 0))[:COLS]


def renew_kernel(
    scal_ref, bound_ref, base_ref, face_ref, mom_ref, tot_ref, kind_ref, mask_ref, table_ref,
    out_ref,
    work_ref, wide_ref, lhs_ref, keep_ref, amp_ref, res_ref, flux_ref,
    *, planes,
):
    n = pl.program_id(0)
    cells = ROWS * ROWS
    inner = (ROWS - 2) * ROWS
    face_y = (planes + 1) * inner
    face_z = face_y + planes * cells
    faces = face_z + planes * inner
    own = planes * cells

    @pl.when(n == 0)
    def _():
        t = [mom_ref[i : i + 1, :] for i in range(COLS)]
        density, velocity, temper, heat = state_of(t)
        tau = relaxation(density, temper)
        heat = [2.0 * tau * q / (2.0 * tau + HALF * PRANDTL) for q in heat]
        divide = 1.0 / (2.0 * tau + HALF)
        keep = 2.0 * tau * divide
        amplitude = (HALF * divide) * (density / (temper * jnp.sqrt(temper)))
        turned = transposed_parts(exponent_coefs(velocity, temper), keep, wide_ref)[:faces]
        lhs_ref[0:faces, :] = turned.astype(jnp.bfloat16)
        keep_ref[...] = spread_column(turned)
        turned = transposed_parts(
            shakhov_coefs(amplitude, density, velocity, temper, heat), None, wide_ref
        )[:faces]
        lhs_ref[faces : 2 * faces, :] = turned.astype(jnp.bfloat16)

        density = tot_ref[0:1, :]
        kind = kind_ref[...]
        inlet, outlet = kind == 2, kind == 3
        moving = [
            jnp.where(outlet, UNIT * tot_ref[1 + e : 2 + e, :] / density, 0.0) for e in range(3)
        ]
        moving[0] = jnp.where(inlet, bound_ref[1], moving[0])
        dense = jnp.where(inlet, bound_ref[0], jnp.where(outlet, bound_ref[3], density))
        warm = jnp.where(inlet, bound_ref[2], jnp.where(outlet, bound_ref[4], bound_ref[5]))
        amplitude = dense / (warm * jnp.sqrt(warm))
        turned = transposed_parts(exponent_coefs(moving, warm), amplitude, work_ref)
        lhs_ref[2 * faces : 2 * faces + own, :] = turned.astype(jnp.bfloat16)
        amp_ref[...] = spread_column(turned)

    res_ref[...] = dot_nn(lhs_ref[...], table_ref[...])

    for r in range(0, faces, 16):
        rows = slice(r, r + 16)
        poly = res_ref[faces + r : faces + r + 16, :]
        flux_ref[rows, :] = (
            twice(keep_ref[rows, :]) * face_ref[rows, :] + jnp.exp2(res_ref[rows, :]) * poly
        )

    along_y, along_z = lane_speeds((ROWS, TILE))
    hy = DT * along_y
    hz = DT * along_z
    digit = scal_ref[1] + n
    hx = (2 * digit + 1 - NODES).astype(jnp.float32) * (UNIT * DT)

    for p in range(planes):
        for y in range(ROWS):
            at = p * cells + y * ROWS
            rows = slice(at, at + ROWS)
            other = twice(amp_ref[rows, :]) * jnp.exp2(
                res_ref[2 * faces + at : 2 * faces + at + ROWS, :]
            )
            if 0 < y < ROWS - 1:
                ax = p * inner + (y - 1) * ROWS
                ay = face_y + at
                az = face_z + ax
                along = flux_ref[ax + inner : ax + inner + ROWS, :] - flux_ref[ax : ax + ROWS, :]
                across = flux_ref[ay + ROWS : ay + 2 * ROWS, :] - flux_ref[ay : ay + ROWS, :]
                low = flux_ref[az : az + ROWS, :]
                rise = pltpu.roll(low, ROWS - 1, 0) - low
                fresh = base_ref[rows, :] - (hx * along + hy * across + hz * rise)
                out_ref[rows, :] = jnp.where(twice(mask_ref[rows, :]) > 0.0, fresh, other)
            else:
                out_ref[rows, :] = other


def on_device(dist, cell_type, boundary, *, spaces, vels):
    planes, across, height, local = dist.shape
    cells = across * height
    own = planes * cells
    inner = cells - 2 * height
    faces = (planes + 1) * inner + planes * cells + planes * inner
    padded = -(-faces // 128) * 128
    slots = planes + 3
    slab_rows = slots * cells
    steps = local // TILE
    space, vel = lax.axis_index("space"), lax.axis_index("vel")
    neg = (vel < vels // 2).astype(jnp.int32)
    scal = jnp.stack([neg, vel * steps]).astype(jnp.int32)
    table = lax.dynamic_slice_in_dim(node_table(), vel * local, local, 1)

    kinds = jnp.pad(cell_type, ((2, 2), (0, 0), (0, 0)))
    kinds = lax.dynamic_slice_in_dim(kinds, space * planes, planes + 4, 0).reshape(-1)
    fluid = jnp.broadcast_to((kinds == 1).astype(jnp.float32)[:, None], (kinds.size, HALFTILE))
    mask_slab = lax.dynamic_slice_in_dim(fluid, neg * cells, slab_rows, 0)
    mask_own = fluid[2 * cells : 2 * cells + own]
    kind_own = kinds[2 * cells : 2 * cells + own].reshape(1, own)

    whole = lambda *shape: pl.BlockSpec(shape, lambda n: (0,) * len(shape))
    tiled = lambda rows: pl.BlockSpec((rows, TILE), lambda n: (0, n))
    smem = pl.BlockSpec(memory_space=pltpu.SMEM)
    f32, bf16 = jnp.float32, jnp.bfloat16
    params = pltpu.CompilerParams(dimension_semantics=("arbitrary",))

    moments = pl.pallas_call(
        moments_kernel,
        grid=(steps,),
        in_specs=[tiled(own), tiled(HALFTILE)],
        out_specs=whole(COLS, own),
        out_shape=jax.ShapeDtypeStruct((COLS, own), f32),
        scratch_shapes=[pltpu.VMEM((own, HALFTILE), f32)],
        compiler_params=params,
        name="moments",
    )
    faces_call = pl.pallas_call(
        functools.partial(faces_kernel, planes=planes),
        grid=(steps,),
        in_specs=[
            smem, tiled(own), tiled(2 * cells), tiled(cells), whole(COLS, own + 4 * cells),
            whole(slab_rows, HALFTILE), tiled(HALFTILE),
        ],
        out_specs=[tiled(own), tiled(faces), whole(COLS, padded)],
        out_shape=[
            jax.ShapeDtypeStruct((own, local), f32),
            jax.ShapeDtypeStruct((faces, local), f32),
            jax.ShapeDtypeStruct((COLS, padded), f32),
        ],
        scratch_shapes=[
            pltpu.VMEM((HALFTILE, own + 4 * cells), f32),
            pltpu.VMEM((own + 4 * cells, HALFTILE), f32),
            pltpu.VMEM((2 * slab_rows, HALFTILE), bf16),
            pltpu.VMEM((slab_rows, HALFTILE), f32),
            pltpu.VMEM((2 * slab_rows, TILE), f32),
            pltpu.VMEM((slots, cells, TILE), f32),
            pltpu.VMEM((faces, TILE), bf16),
            pltpu.VMEM((faces, TILE), bf16),
            pltpu.VMEM((padded, HALFTILE), f32),
        ],
        compiler_params=params,
        name="faces",
    )
    renew = pl.pallas_call(
        functools.partial(renew_kernel, planes=planes),
        grid=(steps,),
        in_specs=[
            smem, smem, tiled(own), tiled(faces), whole(COLS, padded), whole(COLS, own),
            whole(1, own), whole(own, HALFTILE), tiled(HALFTILE),
        ],
        out_specs=tiled(own),
        out_shape=jax.ShapeDtypeStruct((own, local), f32),
        scratch_shapes=[
            pltpu.VMEM((HALFTILE, own), f32),
            pltpu.VMEM((HALFTILE, padded), f32),
            pltpu.VMEM((2 * faces + own, HALFTILE), bf16),
            pltpu.VMEM((faces, HALFTILE), f32),
            pltpu.VMEM((own, HALFTILE), f32),
            pltpu.VMEM((2 * faces + own, TILE), f32),
            pltpu.VMEM((faces, TILE), f32),
        ],
        compiler_params=params,
        name="renew",
    )

    upwind, downwind = [], []
    for s in range(spaces - 1):
        for v in range(vels):
            ahead = (s * vels + v, (s + 1) * vels + v)
            back = (ahead[1], ahead[0])
            upwind.append(back if v < vels // 2 else ahead)
            downwind.append(ahead if v < vels // 2 else back)
    rising = [(s, s + 1) for s in range(spaces - 1)]
    falling = [(s + 1, s) for s in range(spaces - 1)]

    def summed(part):
        if vels == 2:
            return part + lax.ppermute(part, "vel", [(0, 1), (1, 0)])
        return lax.psum(part, "vel")

    x = dist.reshape(own, local)
    up_start = jnp.where(neg == 1, 0, own - 2 * cells)
    down_start = jnp.where(neg == 1, own - cells, 0)
    for turn in range(STEPS):
        both = ("space", "vel")
        upw = lax.ppermute(lax.dynamic_slice_in_dim(x, up_start, 2 * cells, 0), both, upwind)
        dn = lax.ppermute(lax.dynamic_slice_in_dim(x, down_start, cells, 0), both, downwind)
        totals = summed(moments(x, table))
        low = lax.ppermute(totals[:, own - 2 * cells :], "space", rising)
        high = lax.ppermute(totals[:, : 2 * cells], "space", falling)
        low = jnp.where(space > 0, low, totals[:, : 2 * cells])
        high = jnp.where(space < spaces - 1, high, totals[:, own - 2 * cells :])
        extended = jnp.concatenate([low, totals, high], axis=1)
        base, face, part = faces_call(scal, x, upw, dn, extended, mask_slab, table)
        x = renew(scal, boundary, base, face, summed(part), totals, kind_own, mask_own, table)
    return x.reshape(planes, across, height, local)


def solution(mesh):
    spaces, vels = mesh.shape["space"], mesh.shape["vel"]
    return jax.shard_map(
        functools.partial(on_device, spaces=spaces, vels=vels),
        mesh=mesh,
        in_specs=(P("space", None, None, "vel"), P(), P()),
        out_specs=P("space", None, None, "vel"),
        check_vma=False,
    )
```

```python
import functools
import math

import jax
import jax.numpy as jnp
import numpy as np
from jax import lax
from jax.experimental import pallas as pl
from jax.experimental.pallas import tpu as pltpu
from jax.sharding import PartitionSpec as P

NODES = 16
STEPS = 2
PRANDTL = 2.0 / 3.0
OMEGA = 0.81
MU_REF = 0.1
DT = 0.1
HALF = 0.05
VMAX = 5.0
SPACING = 2.0 * VMAX / NODES
UNIT = 0.5 * SPACING
WEIGHT = SPACING**3 / (2.0 * math.pi) ** 1.5
LOG2E = 1.4426950408889634
COLS = 16
TILE = NODES * NODES
ROWS = 8
HALFTILE = 128
VMEM_LIMIT = 24 * 2**20


def node_table():
    number = np.arange(NODES**3)
    digits = (number // (NODES * NODES), number // NODES % NODES, number % NODES)
    m = [2 * d + 1 - NODES for d in digits]
    n = m[0] * m[0] + m[1] * m[1] + m[2] * m[2]
    third = [c * n for c in m]
    high = [((v + 32) // 64) * 64 for v in third]
    low = [v - h for v, h in zip(third, high)]
    base = [np.ones_like(n), *m, m[0] * m[0], m[1] * m[1], m[2] * m[2]]
    base += [m[0] * m[1], m[0] * m[2], m[1] * m[2], *high, *low]
    table = np.zeros((HALFTILE, NODES**3), np.float32)
    for part in range(3):
        table[part * COLS : (part + 1) * COLS] = np.stack(base)
    return jnp.asarray(table, jnp.bfloat16)


def dot_nt(a, b):
    return lax.dot_general(a, b, (((1,), (1,)), ((), ())), preferred_element_type=jnp.float32)


def dot_nn(a, b):
    return lax.dot_general(a, b, (((1,), (0,)), ((), ())), preferred_element_type=jnp.float32)


def split(value):
    high = value.astype(jnp.bfloat16)
    low = (value - high.astype(jnp.float32)).astype(jnp.bfloat16)
    return high, low


def state_of(t):
    density = t[0]
    second_unit = UNIT * UNIT
    velocity = [UNIT * t[1 + e] / density for e in range(3)]
    second = (
        (second_unit * t[4], second_unit * t[7], second_unit * t[8]),
        (second_unit * t[7], second_unit * t[5], second_unit * t[9]),
        (second_unit * t[8], second_unit * t[9], second_unit * t[6]),
    )
    trace = second[0][0] + second[1][1] + second[2][2]
    speed_sq = velocity[0] * velocity[0] + velocity[1] * velocity[1] + velocity[2] * velocity[2]
    temper = (trace / density - speed_sq) / 3.0
    heat = [
        0.5
        * (
            (UNIT**3) * (t[10 + e] + t[13 + e])
            - 2.0
            * (
                second[e][0] * velocity[0]
                + second[e][1] * velocity[1]
                + second[e][2] * velocity[2]
            )
            - velocity[e] * trace
            + 2.0 * density * velocity[e] * speed_sq
        )
        for e in range(3)
    ]
    return density, velocity, temper, heat


def relaxation(density, temper):
    return MU_REF * jnp.exp(OMEGA * jnp.log(temper)) / (density * temper)


def exponent_coefs(velocity, temper):
    g = -0.5 * LOG2E / temper
    speed_sq = velocity[0] * velocity[0] + velocity[1] * velocity[1] + velocity[2] * velocity[2]
    square = g * (UNIT * UNIT)
    zero = jnp.zeros_like(g)
    linear = [(-2.0 * UNIT) * g * velocity[e] for e in range(3)]
    return [g * speed_sq, *linear, square, square, square] + [zero] * 9


def shakhov_coefs(amplitude, density, velocity, temper, heat):
    factor = (1.0 - PRANDTL) / (5.0 * density * temper * temper)
    af = amplitude * factor
    inverse = 1.0 / temper
    along = velocity[0] * heat[0] + velocity[1] * heat[1] + velocity[2] * heat[2]
    speed_sq = velocity[0] * velocity[0] + velocity[1] * velocity[1] + velocity[2] * velocity[2]
    a2 = (UNIT * UNIT) * inverse
    b = [(-2.0 * UNIT) * velocity[e] * inverse for e in range(3)]
    c = speed_sq * inverse - 5.0
    kq = [UNIT * heat[e] for e in range(3)]
    cubic = [af * (kq[e] * a2) for e in range(3)]
    return [
        amplitude - af * (along * c),
        *[af * (kq[e] * c - along * b[e]) for e in range(3)],
        *[af * (kq[e] * b[e] - along * a2) for e in range(3)],
        af * (kq[0] * b[1] + kq[1] * b[0]),
        af * (kq[0] * b[2] + kq[2] * b[0]),
        af * (kq[1] * b[2] + kq[2] * b[1]),
        *cubic,
        *cubic,
    ]


def transposed_parts(coefs, extras, work):
    work[...] = jnp.zeros(work.shape, jnp.float32)
    for row, value in enumerate(coefs):
        high = value.astype(jnp.bfloat16).astype(jnp.float32)
        rest = value - high
        middle = rest.astype(jnp.bfloat16).astype(jnp.float32)
        work[row : row + 1, :] = high
        work[COLS + row : COLS + row + 1, :] = middle
        work[2 * COLS + row : 2 * COLS + row + 1, :] = rest - middle
    for row, value in enumerate(extras):
        work[3 * COLS + row : 3 * COLS + row + 1, :] = value
    return jnp.transpose(work[...], (1, 0))


def spread_column(matrix, extra=0):
    at = 3 * COLS + extra
    return jnp.broadcast_to(matrix[:, at : at + 1], (matrix.shape[0], HALFTILE))


def tile_lanes(n):
    return pl.ds(pl.multiple_of(n * TILE, TILE), TILE)


def twice(value):
    return jnp.concatenate([value, value], axis=1)


def lane_speeds(shape):
    lane = lax.broadcasted_iota(jnp.int32, shape, 1)
    along_y = (2 * (lane // NODES) + 1 - NODES).astype(jnp.float32) * UNIT
    along_z = (2 * (lane % NODES) + 1 - NODES).astype(jnp.float32) * UNIT
    return along_y, along_z


def add_sends(scal_ref, x_ref, up_ref, down_ref, lanes):
    inner = down_ref.shape[0]
    far = pl.multiple_of(scal_ref[2], ROWS)
    near = pl.multiple_of(scal_ref[3], ROWS)
    down = pl.multiple_of(scal_ref[6], ROWS)
    up_ref[:inner, lanes] = x_ref[pl.ds(far, inner), lanes]
    up_ref[inner:, lanes] = x_ref[pl.ds(near, up_ref.shape[0] - inner), lanes]
    down_ref[:, lanes] = x_ref[pl.ds(down, inner), lanes]


def unroll_of(tiles):
    return 2 if tiles % 2 == 0 else 1


def moments_kernel(
    scal_ref, x_ref, kind_ref, table_ref, out_ref, up_ref, down_ref, mask_ref, acc_ref, work_ref
):
    acc_ref[...] = jnp.zeros_like(acc_ref)

    @pl.loop(0, x_ref.shape[1] // TILE)
    def _(n):
        lanes = tile_lanes(n)
        high, low = split(x_ref[:, lanes])
        table = table_ref[:, tile_lanes(scal_ref[1] + n)]
        acc_ref[...] += dot_nt(high, table) + dot_nt(low, table)
        add_sends(scal_ref, x_ref, up_ref, down_ref, lanes)

    out_ref[...] = WEIGHT * jnp.transpose(acc_ref[...], (1, 0))[:COLS]
    fluid = (kind_ref[...] == 1).astype(jnp.float32)
    mask_ref[...] = spread_column(transposed_parts([], [fluid], work_ref))


def cell_coefs(t):
    density, velocity, temper, heat = state_of(t)
    tau = relaxation(density, temper)
    heat = [q / (1.0 + DT * PRANDTL / (2.0 * tau)) for q in heat]
    divide = 1.0 / (2.0 * tau + DT)
    alpha = (2.0 * tau - HALF) * divide
    beta = (3.0 * HALF) * divide
    amplitude = beta * (density / (temper * jnp.sqrt(temper)))
    poly = shakhov_coefs(amplitude, density, velocity, temper, heat)
    return exponent_coefs(velocity, temper), poly, alpha


def middle(a, b):
    return jnp.maximum(jnp.minimum(a, b), jnp.minimum(jnp.maximum(a, b), 0.0))


class Lanes:
    def __init__(self):
        along_y, along_z = lane_speeds((ROWS, TILE))
        lane = lax.broadcasted_iota(jnp.int32, (ROWS, TILE), 1)
        self.z_minus = (lane % NODES) < NODES // 2
        self.ky = HALF * along_y
        self.kz = HALF * along_z
        self.hy = jnp.where(lane < HALFTILE, -0.5, 0.5)
        self.hz = jnp.where(self.z_minus, -0.5, 0.5)


def put_faces(face_ref, part_ref, lanes, first, row, pair):
    both = jnp.concatenate(pair, axis=0)
    high, low = split(both)
    rows = slice(row, row + 2 * ROWS)
    face_ref[rows, lanes] = both
    part_ref[rows, first : first + TILE] = high
    part_ref[rows, first + TILE : first + 2 * TILE] = low


def plane_faces(col, ahead, behind, mask_of, kx, hx, node, put, rows_x, rows_y, rows_z):
    values = {0: col(0), 1: col(1)}
    diff = values[1] - values[0]
    own = rows_y is not None
    fx, fy, fz = {}, {0: values[0]}, {}
    for y in range(1, ROWS - 1):
        here = values[y]
        values[y + 1] = col(y + 1)
        back, diff = diff, values[y + 1] - here
        mask = mask_of(y)
        slope_y = middle(diff, back) * mask
        slope_x = mask * middle(ahead(y) - here, here - behind(y))
        step = here - pltpu.roll(here, 1, 0)
        slope_z = middle(pltpu.roll(step, ROWS - 1, 0), step) * mask
        centre = here - (kx * slope_x + node.ky * slope_y + node.kz * slope_z)
        fx[y] = centre + hx * slope_x
        if own:
            fy[y] = centre + node.hy * slope_y
            side = centre + node.hz * slope_z
            fz[y] = jnp.where(node.z_minus, side, pltpu.roll(side, 1, 0))
    for i in range((ROWS - 2) // 2):
        put(rows_x + 16 * i, [fx[1 + 2 * i], fx[2 + 2 * i]])
    if own:
        fy[ROWS - 1] = values[ROWS - 1]
        gy = [fy[0]]
        for j in range(1, ROWS):
            gy.append(jnp.concatenate([fy[j][:, :HALFTILE], fy[j - 1][:, HALFTILE:]], axis=1))
        for i in range(ROWS // 2):
            put(rows_y + 16 * i, [gy[2 * i], gy[2 * i + 1]])
        for i in range((ROWS - 2) // 2):
            put(rows_z + 16 * i, [fz[1 + 2 * i], fz[2 + 2 * i]])


def x_factors(scal_ref, n):
    along_x = (2 * (scal_ref[1] + n) + 1 - NODES).astype(jnp.float32) * UNIT
    return HALF * along_x, jnp.where(along_x > 0, 0.5, -0.5)


def stacked_tables(tables):
    return jnp.concatenate([t for t in tables for _ in range(2)], axis=1)


def inner_kernel(
    scal_ref, x_ref, tot_ref, mask_ref, table_ref,
    cell_ref, face_ref, acc_ref,
    work_ref, lhs_ref, alpha_ref, part_ref, *res_refs,
    planes,
):
    cells = ROWS * ROWS
    inner = (ROWS - 2) * ROWS
    own = planes * cells
    count = planes - 2
    unroll = len(res_refs)
    exponent, poly, alpha = cell_coefs([tot_ref[i : i + 1, :] for i in range(COLS)])
    turned = transposed_parts(exponent, [alpha], work_ref)
    lhs_ref[0:own, :] = turned.astype(jnp.bfloat16)
    alpha_ref[...] = spread_column(turned)
    lhs_ref[own : 2 * own, :] = transposed_parts(poly, [], work_ref).astype(jnp.bfloat16)
    acc_ref[...] = jnp.zeros_like(acc_ref)
    node = Lanes()

    @pl.loop(0, x_ref.shape[1] // (TILE * unroll))
    def _(m):
        tables = []
        for k, res_ref in enumerate(res_refs):
            n = m * unroll + k
            lanes = tile_lanes(n)
            table = table_ref[:, tile_lanes(scal_ref[1] + n)]
            tables.append(table)
            res_ref[...] = dot_nn(lhs_ref[...], table)
        for k, res_ref in enumerate(res_refs):
            n = m * unroll + k
            lanes = tile_lanes(n)
            kx, hx = x_factors(scal_ref, n)
            for r in range(0, own, 16):
                rows = slice(r, r + 16)
                cell_ref[rows, lanes] = twice(alpha_ref[rows, :]) * x_ref[rows, lanes] + jnp.exp2(
                    res_ref[rows, :]
                ) * res_ref[own + r : own + r + 16, :]
            put = functools.partial(put_faces, face_ref, part_ref, lanes, 2 * TILE * k)
            for i in range(count):
                base = (i + 1) * cells

                def col(y, base=base):
                    return cell_ref[base + y * ROWS : base + (y + 1) * ROWS, lanes]

                def mask_of(y, base=base):
                    at = 2 * cells + base + y * ROWS
                    return twice(mask_ref[at : at + ROWS, :])

                plane_faces(
                    col,
                    lambda y, base=base: col(y, base + cells),
                    lambda y, base=base: col(y, base - cells),
                    mask_of, kx, hx, node, put,
                    i * inner, count * inner + i * cells, count * (inner + cells) + i * inner,
                )
        acc_ref[...] += dot_nt(part_ref[...], stacked_tables(tables))


def outer_kernel(
    scal_ref, cell_ref, upw_ref, dn_ref, below_ref, above_ref, tot_ref, mask_ref, table_ref,
    inacc_ref,
    face_ref, mom_ref,
    ext_ref, work_ref, full_ref, lhs_ref, alpha_ref, slab_ref, part_ref, acc_ref, sum_ref,
    *res_refs, planes,
):
    neg = scal_ref[0]
    cells = ROWS * ROWS
    inner = (ROWS - 2) * ROWS
    own = planes * cells
    count = planes - 2
    ghosts = cells + 2 * inner
    unroll = len(res_refs)

    ext_ref[:, : 2 * cells] = jnp.where(scal_ref[4] > 0, below_ref[...], tot_ref[:, : 2 * cells])
    ext_ref[:, 2 * cells :] = jnp.where(
        scal_ref[5] > 0, above_ref[...], tot_ref[:, own - 2 * cells :]
    )
    exponent, poly, alpha = cell_coefs([ext_ref[i : i + 1, :] for i in range(COLS)])
    near = pl.ds(pl.multiple_of((1 + neg) * cells, ROWS), cells)
    far = pl.ds(pl.multiple_of(3 * neg * cells + ROWS, ROWS), inner)
    down = pl.ds(pl.multiple_of((2 - neg) * cells + ROWS, ROWS), inner)

    def gather():
        return jnp.concatenate([full_ref[far, :], full_ref[near, :], full_ref[down, :]], axis=0)

    full_ref[...] = transposed_parts(exponent, [alpha], work_ref)
    turned = gather()
    lhs_ref[0:ghosts, :] = turned.astype(jnp.bfloat16)
    alpha_ref[...] = spread_column(turned)
    full_ref[...] = transposed_parts(poly, [], work_ref)
    lhs_ref[ghosts : 2 * ghosts, :] = gather().astype(jnp.bfloat16)
    acc_ref[...] = jnp.zeros_like(acc_ref)
    node = Lanes()
    minus = neg > 0
    near_mask = pl.multiple_of((1 + (planes + 1) * neg) * cells, ROWS)

    @pl.loop(0, cell_ref.shape[1] // (TILE * unroll))
    def _(m):
        tables = []
        for k, res_ref in enumerate(res_refs):
            n = m * unroll + k
            table = table_ref[:, tile_lanes(scal_ref[1] + n)]
            tables.append(table)
            res_ref[...] = dot_nn(lhs_ref[...], table)
        for k, res_ref in enumerate(res_refs):
            n = m * unroll + k
            lanes = tile_lanes(n)
            kx, hx = x_factors(scal_ref, n)
            for r in range(0, ghosts, 16):
                rows = slice(r, r + 16)
                if r < inner + cells:
                    f = upw_ref[rows, lanes]
                else:
                    f = dn_ref[r - inner - cells : r - inner - cells + 16, lanes]
                slab_ref[rows, k * TILE : (k + 1) * TILE] = twice(alpha_ref[rows, :]) * f + jnp.exp2(
                    res_ref[rows, :]
                ) * res_ref[ghosts + r : ghosts + r + 16, :]
            put = functools.partial(put_faces, face_ref, part_ref, lanes, 2 * TILE * k)

            def ghost(first, y):
                at = first + y * ROWS
                return slab_ref[at : at + ROWS, k * TILE : (k + 1) * TILE]

            far_at = functools.partial(ghost, -ROWS)
            near_at = functools.partial(ghost, inner)
            down_at = functools.partial(ghost, inner + cells - ROWS)

            def cell(plane, y):
                at = plane * cells + y * ROWS
                return cell_ref[at : at + ROWS, lanes]

            def cell_mask(plane, y):
                at = (2 + plane) * cells + y * ROWS
                return twice(mask_ref[at : at + ROWS, :])

            def ghost_mask(y):
                at = pl.multiple_of(near_mask + y * ROWS, ROWS)
                return twice(mask_ref[pl.ds(at, ROWS), :])

            end = planes - 1
            plane_faces(
                near_at,
                lambda y: jnp.where(minus, cell(end, y), cell(0, y)),
                far_at,
                ghost_mask, jnp.abs(kx), 0.5, node, put, 0, None, None,
            )
            plane_faces(
                functools.partial(cell, 0),
                functools.partial(cell, 1),
                lambda y: jnp.where(minus, down_at(y), near_at(y)),
                functools.partial(cell_mask, 0), kx, hx, node, put,
                inner, 3 * inner, 3 * inner + 2 * cells,
            )
            plane_faces(
                functools.partial(cell, end),
                lambda y: jnp.where(minus, near_at(y), down_at(y)),
                functools.partial(cell, end - 1),
                functools.partial(cell_mask, end), kx, hx, node, put,
                2 * inner, 3 * inner + cells, 4 * inner + 2 * cells,
            )
        acc_ref[...] += dot_nt(part_ref[...], stacked_tables(tables))

    face_y = (planes + 1) * inner
    face_z = face_y + planes * cells
    used = face_z + planes * inner
    if sum_ref.shape[0] > used:
        sum_ref[used:, :] = jnp.zeros((sum_ref.shape[0] - used, HALFTILE), jnp.float32)

    def place(row, size, source, at):
        sum_ref[pl.ds(pl.multiple_of(row, ROWS), size), :] = source[at : at + size, :]

    place(planes * neg * inner, inner, acc_ref, 0)
    for p in range(planes):
        outer = p in (0, planes - 1)
        source = acc_ref if outer else inacc_ref
        i = (0 if p == 0 else 1) if outer else p - 1
        size = 2 if outer else count
        skip = inner if outer else 0
        place((p + 1 - neg) * inner, inner, source, skip + i * inner)
        place(face_y + p * cells, cells, source, skip + size * inner + i * cells)
        place(face_z + p * inner, inner, source, skip + size * (inner + cells) + i * inner)
    mom_ref[...] = WEIGHT * jnp.transpose(sum_ref[...], (1, 0))[:COLS]


def renew_kernel(
    scal_ref, bound_ref, x_ref, cell_ref, in_ref, edge_ref, mom_ref, peer_ref, tot_ref, kind_ref,
    mask_ref, table_ref,
    *refs, planes, last, unroll,
):
    if last:
        out_ref, *refs = refs
    else:
        out_ref, next_ref, up_ref, down_ref, *refs = refs
    work_ref, wide_ref, lhs_ref, keep_ref, amp_ref, acc_ref, part_ref, *refs = refs
    res_refs, flux_refs = refs[:unroll], refs[unroll:]
    minus = scal_ref[0] > 0
    cells = ROWS * ROWS
    inner = (ROWS - 2) * ROWS
    count = planes - 2
    face_y = (planes + 1) * inner
    face_z = face_y + planes * cells
    faces = face_z + planes * inner
    own = planes * cells

    t = [mom_ref[i : i + 1, :] + peer_ref[i : i + 1, :] for i in range(COLS)]
    density, velocity, temper, heat = state_of(t)
    tau = relaxation(density, temper)
    heat = [2.0 * tau * q / (2.0 * tau + HALF * PRANDTL) for q in heat]
    divide = 1.0 / (2.0 * tau + HALF)
    keep = 2.0 * tau * divide
    amplitude = (HALF * divide) * (density / (temper * jnp.sqrt(temper)))
    turned = transposed_parts(exponent_coefs(velocity, temper), [keep], wide_ref)[:faces]
    lhs_ref[0:faces, :] = turned.astype(jnp.bfloat16)
    keep_ref[...] = spread_column(turned)
    turned = transposed_parts(
        shakhov_coefs(amplitude, density, velocity, temper, heat), [], wide_ref
    )[:faces]
    lhs_ref[faces : 2 * faces, :] = turned.astype(jnp.bfloat16)

    density = tot_ref[0:1, :]
    kind = kind_ref[:, 2 * cells : 2 * cells + own]
    inlet, outlet = kind == 2, kind == 3
    moving = [
        jnp.where(outlet, UNIT * tot_ref[1 + e : 2 + e, :] / density, 0.0) for e in range(3)
    ]
    moving[0] = jnp.where(inlet, bound_ref[1], moving[0])
    dense = jnp.where(inlet, bound_ref[0], jnp.where(outlet, bound_ref[3], density))
    warm = jnp.where(inlet, bound_ref[2], jnp.where(outlet, bound_ref[4], bound_ref[5]))
    amplitude = dense / (warm * jnp.sqrt(warm))
    turned = transposed_parts(exponent_coefs(moving, warm), [amplitude], work_ref)
    lhs_ref[2 * faces : 2 * faces + own, :] = turned.astype(jnp.bfloat16)
    amp_ref[...] = spread_column(turned)
    acc_ref[...] = jnp.zeros_like(acc_ref)

    along_y, along_z = lane_speeds((ROWS, TILE))
    hy = DT * along_y
    hz = DT * along_z

    def along_x_source(plane):
        if plane in (-1, planes):
            return edge_ref, 0
        if plane in (0, planes - 1):
            return edge_ref, inner if plane == 0 else 2 * inner
        return in_ref, (plane - 1) * inner

    def face_rows(r, lanes):
        rows = 2 * ROWS

        def load(ref, at):
            return ref[at : at + rows, lanes]

        if r < face_y:
            w, rest = divmod(r, inner)
            ref, at = along_x_source(w)
            other, there = along_x_source(w - 1)
            return jnp.where(minus, load(ref, at + rest), load(other, there + rest))
        size, start = (cells, face_y) if r < face_z else (inner, face_z)
        p, rest = divmod(r - start, size)
        outer = p in (0, planes - 1)
        i = (0 if p == 0 else 1) if outer else p - 1
        many, skip = (2, inner) if outer else (count, 0)
        before = skip + many * (inner if r < face_z else inner + cells)
        return load(edge_ref if outer else in_ref, before + i * size + rest)

    @pl.loop(0, x_ref.shape[1] // (TILE * unroll))
    def _(m):
        tables = []
        for k, res_ref in enumerate(res_refs):
            n = m * unroll + k
            table = table_ref[:, tile_lanes(scal_ref[1] + n)]
            tables.append(table)
            res_ref[...] = dot_nn(lhs_ref[...], table)
        for k, (res_ref, flux_ref) in enumerate(zip(res_refs, flux_refs)):
            n = m * unroll + k
            lanes = tile_lanes(n)
            digit = scal_ref[1] + n
            hx = (2 * digit + 1 - NODES).astype(jnp.float32) * (UNIT * DT)
            for r in range(0, faces, 16):
                rows = slice(r, r + 16)
                poly = res_ref[faces + r : faces + r + 16, :]
                flux_ref[rows, :] = (
                    twice(keep_ref[rows, :]) * face_rows(r, lanes) + jnp.exp2(res_ref[rows, :]) * poly
                )
            for p in range(planes):
                done = []
                for y in range(ROWS):
                    at = p * cells + y * ROWS
                    rows = slice(at, at + ROWS)
                    value = twice(amp_ref[rows, :]) * jnp.exp2(
                        res_ref[2 * faces + at : 2 * faces + at + ROWS, :]
                    )
                    if 0 < y < ROWS - 1:
                        ax = p * inner + (y - 1) * ROWS
                        ay = face_y + at
                        az = face_z + ax
                        along = (
                            flux_ref[ax + inner : ax + inner + ROWS, :]
                            - flux_ref[ax : ax + ROWS, :]
                        )
                        across = (
                            flux_ref[ay + ROWS : ay + 2 * ROWS, :] - flux_ref[ay : ay + ROWS, :]
                        )
                        low = flux_ref[az : az + ROWS, :]
                        rise = pltpu.roll(low, ROWS - 1, 0) - low
                        plus = (4.0 / 3.0) * cell_ref[rows, lanes] - (1.0 / 3.0) * x_ref[rows, lanes]
                        fresh = plus - (hx * along + hy * across + hz * rise)
                        at += 2 * cells
                        mask = twice(mask_ref[at : at + ROWS, :]) > 0.0
                        value = jnp.where(mask, fresh, value)
                    done.append(value)
                    if y % 2:
                        both = jnp.concatenate(done, axis=0)
                        rows = slice(p * cells + (y - 1) * ROWS, p * cells + (y + 1) * ROWS)
                        out_ref[rows, lanes] = both
                        if not last:
                            high, low = split(both)
                            first = 2 * TILE * k
                            part_ref[rows, first : first + TILE] = high
                            part_ref[rows, first + TILE : first + 2 * TILE] = low
                        done = []
        if not last:
            acc_ref[...] += dot_nt(part_ref[...], stacked_tables(tables))
            for k in range(unroll):
                add_sends(scal_ref, out_ref, up_ref, down_ref, tile_lanes(m * unroll + k))

    if not last:
        next_ref[...] = WEIGHT * jnp.transpose(acc_ref[...], (1, 0))[:COLS]


def on_device(dist, cell_type, boundary, *, spaces, vels):
    planes, across, height, local = dist.shape
    cells = across * height
    own = planes * cells
    inner = cells - 2 * height
    faces = (planes + 1) * inner + planes * cells + planes * inner
    padded = -(-faces // 128) * 128
    extended = own + 4 * cells
    ghosts = cells + 2 * inner
    faces_in = (planes - 2) * (2 * inner + cells)
    faces_edge = inner + 2 * (2 * inner + cells)
    tiles = local // TILE
    unroll = unroll_of(tiles)
    space, vel = lax.axis_index("space"), lax.axis_index("vel")
    neg = (vel < vels // 2).astype(jnp.int32)
    scal = jnp.stack(
        [
            neg,
            vel * tiles,
            height + jnp.where(neg == 1, cells, own - 2 * cells),
            jnp.where(neg == 1, 0, own - cells),
            (space > 0).astype(jnp.int32),
            (space < spaces - 1).astype(jnp.int32),
            height + jnp.where(neg == 1, own - cells, 0),
        ]
    ).astype(jnp.int32)
    table = node_table()
    kinds = jnp.pad(cell_type, ((2, 2), (0, 0), (0, 0)))
    kinds = lax.dynamic_slice_in_dim(kinds, space * planes, planes + 4, 0).reshape(1, extended)

    smem = pl.BlockSpec(memory_space=pltpu.SMEM)
    vmem = pl.BlockSpec(memory_space=pltpu.VMEM)
    f32, bf16 = jnp.float32, jnp.bfloat16
    shape = lambda *dims: jax.ShapeDtypeStruct(dims, f32)
    scratch = lambda *dims: pltpu.VMEM(dims, f32)
    packed = lambda *dims: pltpu.VMEM(dims, bf16)
    params = pltpu.CompilerParams(vmem_limit_bytes=VMEM_LIMIT)
    cost = lambda us: pl.CostEstimate(
        flops=int(us * 1e9), bytes_accessed=1 << 20, transcendentals=0
    )
    sends = [shape(COLS, own), shape(inner + cells, local), shape(inner, local)]

    moments = pl.pallas_call(
        moments_kernel,
        in_specs=[smem] + [vmem] * 3,
        out_specs=[vmem] * 4,
        out_shape=sends + [shape(extended, HALFTILE)],
        scratch_shapes=[scratch(own, HALFTILE), scratch(HALFTILE, extended)],
        compiler_params=params,
        cost_estimate=cost(2),
        name="moments",
    )
    inside = pl.pallas_call(
        functools.partial(inner_kernel, planes=planes),
        in_specs=[smem] + [vmem] * 4,
        out_specs=[vmem] * 3,
        out_shape=[shape(own, local), shape(faces_in, local), shape(faces_in, HALFTILE)],
        scratch_shapes=[
            scratch(HALFTILE, own),
            packed(2 * own, HALFTILE),
            scratch(own, HALFTILE),
            packed(faces_in, 2 * TILE * unroll),
        ]
        + [scratch(2 * own, TILE)] * unroll,
        compiler_params=params,
        cost_estimate=cost(6),
        name="facesin",
    )
    outside = pl.pallas_call(
        functools.partial(outer_kernel, planes=planes),
        in_specs=[smem] + [vmem] * 9,
        out_specs=[vmem] * 2,
        out_shape=[shape(faces_edge, local), shape(COLS, padded)],
        scratch_shapes=[
            scratch(COLS, 4 * cells),
            scratch(HALFTILE, 4 * cells),
            scratch(4 * cells, HALFTILE),
            packed(2 * ghosts, HALFTILE),
            scratch(ghosts, HALFTILE),
            scratch(ghosts, TILE * unroll),
            packed(faces_edge, 2 * TILE * unroll),
            scratch(faces_edge, HALFTILE),
            scratch(padded, HALFTILE),
        ]
        + [scratch(2 * ghosts, TILE)] * unroll,
        compiler_params=params,
        cost_estimate=cost(6),
        name="faceb",
    )

    def renew(last):
        return pl.pallas_call(
            functools.partial(renew_kernel, planes=planes, last=last, unroll=unroll),
            in_specs=[smem, smem] + [vmem] * 10,
            out_specs=[vmem] * (1 if last else 4),
            out_shape=[shape(own, local)] + ([] if last else sends),
            scratch_shapes=[
                scratch(HALFTILE, own),
                scratch(HALFTILE, padded),
                packed(2 * faces + own, HALFTILE),
                scratch(faces, HALFTILE),
                scratch(own, HALFTILE),
                scratch(own, HALFTILE),
                packed(own, 2 * TILE * unroll),
            ]
            + [scratch(2 * faces + own, TILE)] * unroll
            + [scratch(faces, TILE)] * unroll,
            compiler_params=params,
            cost_estimate=cost(6),
            name="renew",
        )

    upwind, downwind = [], []
    for s in range(spaces - 1):
        for v in range(vels):
            ahead = (s * vels + v, (s + 1) * vels + v)
            back = (ahead[1], ahead[0])
            upwind.append(back if v < vels // 2 else ahead)
            downwind.append(ahead if v < vels // 2 else back)
    rising = [(s, s + 1) for s in range(spaces - 1)]
    falling = [(s + 1, s) for s in range(spaces - 1)]
    both = ("space", "vel")

    def others(part):
        if vels == 2:
            return lax.ppermute(part, "vel", [(0, 1), (1, 0)])
        return lax.psum(part, "vel") - part

    x = dist.reshape(own, local)
    part, up, down, mask = moments(scal, x, kinds, table)
    for turn in range(STEPS):
        last = turn == STEPS - 1
        upw = lax.ppermute(up, both, upwind)
        dn = lax.ppermute(down, both, downwind)
        totals = part + others(part)
        below = lax.ppermute(totals[:, own - 2 * cells :], "space", rising)
        above = lax.ppermute(totals[:, : 2 * cells], "space", falling)
        cell, face_in, sums = inside(scal, x, totals, mask, table)
        face_edge, part = outside(
            scal, cell, upw, dn, below, above, totals, mask, table, sums
        )
        out = renew(last)(
            scal, boundary, x, cell, face_in, face_edge, part, others(part), totals, kinds, mask,
            table,
        )
        if last:
            (x,) = out
        else:
            x, part, up, down = out
    return x.reshape(planes, across, height, local)


def solution(mesh):
    spaces, vels = mesh.shape["space"], mesh.shape["vel"]
    return jax.shard_map(
        functools.partial(on_device, spaces=spaces, vels=vels),
        mesh=mesh,
        in_specs=(P("space", None, None, "vel"), P(), P()),
        out_specs=P("space", None, None, "vel"),
        check_vma=False,
    )
```

```python
import functools
import math

import jax
import jax.numpy as jnp
import numpy as np
from jax import lax
from jax.experimental import pallas as pl
from jax.experimental.pallas import tpu as pltpu
from jax.sharding import PartitionSpec as P

NODES = 16
STEPS = 2
PRANDTL = 2.0 / 3.0
OMEGA = 0.81
MU_REF = 0.1
DT = 0.1
HALF = 0.05
VMAX = 5.0
SPACING = 2.0 * VMAX / NODES
UNIT = 0.5 * SPACING
WEIGHT = SPACING**3 / (2.0 * math.pi) ** 1.5
LOG2E = 1.4426950408889634
COLS = 16
TILE = NODES * NODES
ROWS = 8
HALFTILE = 128
KEYS = 64
VMEM_LIMIT = 24 * 2**20


def node_table():
    number = np.arange(NODES**3)
    digits = (number // (NODES * NODES), number // NODES % NODES, number % NODES)
    m = [2 * d + 1 - NODES for d in digits]
    n = m[0] * m[0] + m[1] * m[1] + m[2] * m[2]
    third = [c * n for c in m]
    high = [((v + 32) // 64) * 64 for v in third]
    low = [v - h for v, h in zip(third, high)]
    base = [np.ones_like(n), *m, m[0] * m[0], m[1] * m[1], m[2] * m[2]]
    base += [m[0] * m[1], m[0] * m[2], m[1] * m[2], *high, *low]
    table = np.zeros((KEYS, NODES**3), np.float32)
    for part in range(3):
        table[part * COLS : (part + 1) * COLS] = np.stack(base)
    return jnp.asarray(table, jnp.bfloat16)


def dot_nt(a, b):
    return lax.dot_general(a, b, (((1,), (1,)), ((), ())), preferred_element_type=jnp.float32)


def dot_nn(a, b):
    return lax.dot_general(a, b, (((1,), (0,)), ((), ())), preferred_element_type=jnp.float32)


def split(value):
    high = value.astype(jnp.bfloat16)
    low = (value - high.astype(jnp.float32)).astype(jnp.bfloat16)
    return high, low


def state_of(t):
    density = t[0]
    second_unit = UNIT * UNIT
    velocity = [UNIT * t[1 + e] / density for e in range(3)]
    second = (
        (second_unit * t[4], second_unit * t[7], second_unit * t[8]),
        (second_unit * t[7], second_unit * t[5], second_unit * t[9]),
        (second_unit * t[8], second_unit * t[9], second_unit * t[6]),
    )
    trace = second[0][0] + second[1][1] + second[2][2]
    speed_sq = velocity[0] * velocity[0] + velocity[1] * velocity[1] + velocity[2] * velocity[2]
    temper = (trace / density - speed_sq) / 3.0
    heat = [
        0.5
        * (
            (UNIT**3) * (t[10 + e] + t[13 + e])
            - 2.0
            * (
                second[e][0] * velocity[0]
                + second[e][1] * velocity[1]
                + second[e][2] * velocity[2]
            )
            - velocity[e] * trace
            + 2.0 * density * velocity[e] * speed_sq
        )
        for e in range(3)
    ]
    return density, velocity, temper, heat


def relaxation(density, temper):
    return MU_REF * jnp.exp(OMEGA * jnp.log(temper)) / (density * temper)


def exponent_coefs(velocity, temper):
    g = -0.5 * LOG2E / temper
    speed_sq = velocity[0] * velocity[0] + velocity[1] * velocity[1] + velocity[2] * velocity[2]
    square = g * (UNIT * UNIT)
    linear = [(-2.0 * UNIT) * g * velocity[e] for e in range(3)]
    return [g * speed_sq, *linear, square, square, square]


def shakhov_coefs(amplitude, density, velocity, temper, heat):
    factor = (1.0 - PRANDTL) / (5.0 * density * temper * temper)
    af = amplitude * factor
    inverse = 1.0 / temper
    along = velocity[0] * heat[0] + velocity[1] * heat[1] + velocity[2] * heat[2]
    speed_sq = velocity[0] * velocity[0] + velocity[1] * velocity[1] + velocity[2] * velocity[2]
    a2 = (UNIT * UNIT) * inverse
    b = [(-2.0 * UNIT) * velocity[e] * inverse for e in range(3)]
    c = speed_sq * inverse - 5.0
    kq = [UNIT * heat[e] for e in range(3)]
    cubic = [af * (kq[e] * a2) for e in range(3)]
    return [
        amplitude - af * (along * c),
        *[af * (kq[e] * c - along * b[e]) for e in range(3)],
        *[af * (kq[e] * b[e] - along * a2) for e in range(3)],
        af * (kq[0] * b[1] + kq[1] * b[0]),
        af * (kq[0] * b[2] + kq[2] * b[0]),
        af * (kq[1] * b[2] + kq[2] * b[1]),
        *cubic,
        *cubic,
    ]


def transposed_parts(coefs, extras, work):
    count = work.shape[1]
    work[0:COLS, :] = jnp.zeros((COLS, count), jnp.float32)
    work[3 * COLS :, :] = jnp.zeros((KEYS - 3 * COLS, count), jnp.float32)
    for row, value in enumerate(coefs):
        work[row : row + 1, :] = value
    for row, value in enumerate(extras):
        work[3 * COLS + row : 3 * COLS + row + 1, :] = value
    value = work[0:COLS, :]
    high = value.astype(jnp.bfloat16).astype(jnp.float32)
    rest = value - high
    middle = rest.astype(jnp.bfloat16).astype(jnp.float32)
    work[0:COLS, :] = high
    work[COLS : 2 * COLS, :] = middle
    work[2 * COLS : 3 * COLS, :] = rest - middle
    return jnp.transpose(work[...], (1, 0))


def spread_column(matrix, extra=0):
    at = 3 * COLS + extra
    return jnp.broadcast_to(matrix[:, at : at + 1], (matrix.shape[0], HALFTILE))


def tile_lanes(n):
    return pl.ds(pl.multiple_of(n * TILE, TILE), TILE)


def twice(value):
    return jnp.concatenate([value, value], axis=1)


def lane_speeds(shape):
    lane = lax.broadcasted_iota(jnp.int32, shape, 1)
    along_y = (2 * (lane // NODES) + 1 - NODES).astype(jnp.float32) * UNIT
    along_z = (2 * (lane % NODES) + 1 - NODES).astype(jnp.float32) * UNIT
    return along_y, along_z


def add_sends(scal_ref, x_ref, up_ref, down_ref, lanes):
    cells = ROWS * ROWS
    short = down_ref.shape[0]

    def pack(plane, ref):
        ref[short - ROWS : short, lanes] = jnp.zeros((ROWS, TILE), jnp.float32)
        for y in range(1, ROWS - 1):
            column = x_ref[pl.ds(pl.multiple_of(plane * cells + y * ROWS, ROWS), ROWS), lanes]
            first = (y - 1) * (ROWS - 2)
            if y == 1:
                ref[0:ROWS, lanes] = column
            else:
                ref[first + 1 : first + ROWS - 1, lanes] = column[1 : ROWS - 1]

    pack(scal_ref[2], up_ref)
    near = pl.multiple_of(scal_ref[3] * cells, ROWS)
    up_ref[short:, lanes] = x_ref[pl.ds(near, cells), lanes]
    pack(scal_ref[6], down_ref)


def sends_kernel(scal_ref, x_ref, up_ref, down_ref):
    @pl.loop(0, x_ref.shape[1] // TILE)
    def _(n):
        add_sends(scal_ref, x_ref, up_ref, down_ref, tile_lanes(n))


def unroll_of(tiles):
    return 8 if tiles % 8 == 0 else 4 if tiles % 4 == 0 else 2 if tiles % 2 == 0 else 1


def moments_kernel(
    scal_ref, x_ref, kind_ref, table_ref, out_ref, mask_ref, acc_ref, work_ref
):
    acc_ref[...] = jnp.zeros_like(acc_ref)

    @pl.loop(0, x_ref.shape[1] // TILE)
    def _(n):
        lanes = tile_lanes(n)
        high, low = split(x_ref[:, lanes])
        table = table_ref[:, tile_lanes(scal_ref[1] + n)]
        acc_ref[...] += dot_nt(high, table) + dot_nt(low, table)

    out_ref[...] = WEIGHT * jnp.transpose(acc_ref[...], (1, 0))[:COLS]
    fluid = (kind_ref[...] == 1).astype(jnp.float32)
    mask_ref[...] = spread_column(transposed_parts([], [fluid], work_ref))


def cell_coefs(t):
    density, velocity, temper, heat = state_of(t)
    tau = relaxation(density, temper)
    heat = [q / (1.0 + DT * PRANDTL / (2.0 * tau)) for q in heat]
    divide = 1.0 / (2.0 * tau + DT)
    alpha = (2.0 * tau - HALF) * divide
    beta = (3.0 * HALF) * divide
    amplitude = beta * (density / (temper * jnp.sqrt(temper)))
    poly = shakhov_coefs(amplitude, density, velocity, temper, heat)
    return exponent_coefs(velocity, temper), poly, alpha


def middle(a, b):
    return jnp.maximum(jnp.minimum(a, b), jnp.minimum(jnp.maximum(a, b), 0.0))


class Lanes:
    def __init__(self):
        along_y, along_z = lane_speeds((ROWS, TILE))
        lane = lax.broadcasted_iota(jnp.int32, (ROWS, TILE), 1)
        self.z_minus = (lane % NODES) < NODES // 2
        self.ky = HALF * along_y
        self.kz = HALF * along_z
        self.hy = jnp.where(lane < HALFTILE, -0.5, 0.5)
        self.hz = jnp.where(self.z_minus, -0.5, 0.5)


def put_faces(face_ref, part_ref, lanes, first, row, pair):
    both = jnp.concatenate(pair, axis=0)
    high, low = split(both)
    rows = slice(row, row + 2 * ROWS)
    face_ref[rows, lanes] = both
    part_ref[rows, first : first + TILE] = high
    part_ref[rows, first + TILE : first + 2 * TILE] = low


def plane_faces(col, ahead, behind, mask_of, kx, hx, node, put, rows_x, rows_y, rows_z):
    values = {0: col(0), 1: col(1)}
    diff = values[1] - values[0]
    own = rows_y is not None
    fx, fy, fz = {}, {0: values[0]}, {}
    for y in range(1, ROWS - 1):
        here = values[y]
        values[y + 1] = col(y + 1)
        back, diff = diff, values[y + 1] - here
        mask = mask_of(y)
        slope_y = middle(diff, back) * mask
        slope_x = mask * middle(ahead(y) - here, here - behind(y))
        step = here - pltpu.roll(here, 1, 0)
        slope_z = middle(pltpu.roll(step, ROWS - 1, 0), step) * mask
        centre = here - (kx * slope_x + node.ky * slope_y + node.kz * slope_z)
        fx[y] = centre + hx * slope_x
        if own:
            fy[y] = centre + node.hy * slope_y
            side = centre + node.hz * slope_z
            fz[y] = jnp.where(node.z_minus, side, pltpu.roll(side, 1, 0))
    for i in range((ROWS - 2) // 2):
        put(rows_x + 16 * i, [fx[1 + 2 * i], fx[2 + 2 * i]])
    if own:
        fy[ROWS - 1] = values[ROWS - 1]
        gy = [fy[0]]
        for j in range(1, ROWS):
            gy.append(jnp.concatenate([fy[j][:, :HALFTILE], fy[j - 1][:, HALFTILE:]], axis=1))
        for i in range(ROWS // 2):
            put(rows_y + 16 * i, [gy[2 * i], gy[2 * i + 1]])
        for i in range((ROWS - 2) // 2):
            put(rows_z + 16 * i, [fz[1 + 2 * i], fz[2 + 2 * i]])


def x_factors(scal_ref, n):
    along_x = (2 * (scal_ref[1] + n) + 1 - NODES).astype(jnp.float32) * UNIT
    return HALF * along_x, jnp.where(along_x > 0, 0.5, -0.5)


def stacked_tables(tables):
    return jnp.concatenate([t for t in tables for _ in range(2)], axis=1)


def inner_kernel(
    scal_ref, x_ref, tot_ref, mask_ref, table_ref,
    cell_ref, face_ref, acc_ref,
    work_ref, lhs_ref, alpha_ref, part_ref, *res_refs,
    planes,
):
    cells = ROWS * ROWS
    inner = (ROWS - 2) * ROWS
    own = planes * cells
    count = planes - 2
    unroll = len(res_refs)
    exponent, poly, alpha = cell_coefs([tot_ref[i : i + 1, :] for i in range(COLS)])
    turned = transposed_parts(exponent, [alpha], work_ref)
    lhs_ref[0:own, :] = turned.astype(jnp.bfloat16)
    alpha_ref[...] = spread_column(turned)
    lhs_ref[own : 2 * own, :] = transposed_parts(poly, [], work_ref).astype(jnp.bfloat16)
    acc_ref[...] = jnp.zeros_like(acc_ref)
    node = Lanes()

    @pl.loop(0, x_ref.shape[1] // (TILE * unroll))
    def _(m):
        tables = []
        for k, res_ref in enumerate(res_refs):
            n = m * unroll + k
            lanes = tile_lanes(n)
            table = table_ref[:, tile_lanes(scal_ref[1] + n)]
            tables.append(table)
            res_ref[...] = dot_nn(lhs_ref[...], table)
        for k, res_ref in enumerate(res_refs):
            n = m * unroll + k
            lanes = tile_lanes(n)
            kx, hx = x_factors(scal_ref, n)
            for r in range(0, own, 16):
                rows = slice(r, r + 16)
                cell_ref[rows, lanes] = twice(alpha_ref[rows, :]) * x_ref[rows, lanes] + jnp.exp2(
                    res_ref[rows, :]
                ) * res_ref[own + r : own + r + 16, :]
            put = functools.partial(put_faces, face_ref, part_ref, lanes, 2 * TILE * k)
            for i in range(count):
                base = (i + 1) * cells

                def col(y, base=base):
                    return cell_ref[base + y * ROWS : base + (y + 1) * ROWS, lanes]

                def mask_of(y, base=base):
                    at = 2 * cells + base + y * ROWS
                    return twice(mask_ref[at : at + ROWS, :])

                plane_faces(
                    col,
                    lambda y, base=base: col(y, base + cells),
                    lambda y, base=base: col(y, base - cells),
                    mask_of, kx, hx, node, put,
                    i * inner, count * inner + i * cells, count * (inner + cells) + i * inner,
                )
        acc_ref[...] += dot_nt(part_ref[...], stacked_tables(tables))


def outer_kernel(
    scal_ref, cell_ref, upw_ref, dn_ref, below_ref, above_ref, tot_ref, mask_ref, table_ref,
    inacc_ref,
    face_ref, mom_ref,
    ext_ref, work_ref, full_ref, lhs_ref, alpha_ref, slab_ref, part_ref, acc_ref, sum_ref,
    *res_refs, planes,
):
    neg = scal_ref[0]
    cells = ROWS * ROWS
    inner = (ROWS - 2) * ROWS
    own = planes * cells
    count = planes - 2
    ghosts = cells + 2 * inner
    unroll = len(res_refs)

    ext_ref[:, : 2 * cells] = jnp.where(scal_ref[4] > 0, below_ref[...], tot_ref[:, : 2 * cells])
    ext_ref[:, 2 * cells :] = jnp.where(
        scal_ref[5] > 0, above_ref[...], tot_ref[:, own - 2 * cells :]
    )
    exponent, poly, alpha = cell_coefs([ext_ref[i : i + 1, :] for i in range(COLS)])
    near = pl.ds(pl.multiple_of((1 + neg) * cells, ROWS), cells)
    far = pl.ds(pl.multiple_of(3 * neg * cells + ROWS, ROWS), inner)
    down = pl.ds(pl.multiple_of((2 - neg) * cells + ROWS, ROWS), inner)

    def gather():
        return jnp.concatenate([full_ref[far, :], full_ref[near, :], full_ref[down, :]], axis=0)

    full_ref[...] = transposed_parts(exponent, [alpha], work_ref)
    turned = gather()
    lhs_ref[0:ghosts, :] = turned.astype(jnp.bfloat16)
    alpha_ref[...] = spread_column(turned)
    full_ref[...] = transposed_parts(poly, [], work_ref)
    lhs_ref[ghosts : 2 * ghosts, :] = gather().astype(jnp.bfloat16)
    acc_ref[...] = jnp.zeros_like(acc_ref)
    node = Lanes()
    minus = neg > 0
    near_mask = pl.multiple_of((1 + (planes + 1) * neg) * cells, ROWS)

    @pl.loop(0, cell_ref.shape[1] // (TILE * unroll))
    def _(m):
        tables = []
        for k, res_ref in enumerate(res_refs):
            n = m * unroll + k
            table = table_ref[:, tile_lanes(scal_ref[1] + n)]
            tables.append(table)
            res_ref[...] = dot_nn(lhs_ref[...], table)
        for k, res_ref in enumerate(res_refs):
            n = m * unroll + k
            lanes = tile_lanes(n)
            kx, hx = x_factors(scal_ref, n)
            for r in range(0, ghosts, 16):
                rows = slice(r, r + 16)
                short = dn_ref.shape[0]
                if inner <= r < inner + cells:
                    f = upw_ref[short + r - inner : short + r - inner + 16, lanes]
                else:
                    ref, y = (upw_ref, r // ROWS) if r < inner else (dn_ref, (r - inner - cells) // ROWS)
                    first = [(y + i) * (ROWS - 2) for i in range(2)]
                    f = jnp.concatenate([ref[a : a + ROWS, lanes] for a in first], axis=0)
                slab_ref[rows, k * TILE : (k + 1) * TILE] = twice(alpha_ref[rows, :]) * f + jnp.exp2(
                    res_ref[rows, :]
                ) * res_ref[ghosts + r : ghosts + r + 16, :]
            put = functools.partial(put_faces, face_ref, part_ref, lanes, 2 * TILE * k)

            def ghost(first, y):
                at = first + y * ROWS
                return slab_ref[at : at + ROWS, k * TILE : (k + 1) * TILE]

            far_at = functools.partial(ghost, -ROWS)
            near_at = functools.partial(ghost, inner)
            down_at = functools.partial(ghost, inner + cells - ROWS)

            def cell(plane, y):
                at = plane * cells + y * ROWS
                return cell_ref[at : at + ROWS, lanes]

            def cell_mask(plane, y):
                at = (2 + plane) * cells + y * ROWS
                return twice(mask_ref[at : at + ROWS, :])

            def ghost_mask(y):
                at = pl.multiple_of(near_mask + y * ROWS, ROWS)
                return twice(mask_ref[pl.ds(at, ROWS), :])

            end = planes - 1
            plane_faces(
                near_at,
                lambda y: jnp.where(minus, cell(end, y), cell(0, y)),
                far_at,
                ghost_mask, jnp.abs(kx), 0.5, node, put, 0, None, None,
            )
            plane_faces(
                functools.partial(cell, 0),
                functools.partial(cell, 1),
                lambda y: jnp.where(minus, down_at(y), near_at(y)),
                functools.partial(cell_mask, 0), kx, hx, node, put,
                inner, 3 * inner, 3 * inner + 2 * cells,
            )
            plane_faces(
                functools.partial(cell, end),
                lambda y: jnp.where(minus, near_at(y), down_at(y)),
                functools.partial(cell, end - 1),
                functools.partial(cell_mask, end), kx, hx, node, put,
                2 * inner, 3 * inner + cells, 4 * inner + 2 * cells,
            )
        acc_ref[...] += dot_nt(part_ref[...], stacked_tables(tables))

    face_y = (planes + 1) * inner
    face_z = face_y + planes * cells
    used = face_z + planes * inner
    if sum_ref.shape[0] > used:
        sum_ref[used:, :] = jnp.zeros((sum_ref.shape[0] - used, KEYS), jnp.float32)

    def place(row, size, source, at):
        sum_ref[pl.ds(pl.multiple_of(row, ROWS), size), :] = source[at : at + size, :]

    place(planes * neg * inner, inner, acc_ref, 0)
    for p in range(planes):
        outer = p in (0, planes - 1)
        source = acc_ref if outer else inacc_ref
        i = (0 if p == 0 else 1) if outer else p - 1
        size = 2 if outer else count
        skip = inner if outer else 0
        place((p + 1 - neg) * inner, inner, source, skip + i * inner)
        place(face_y + p * cells, cells, source, skip + size * inner + i * cells)
        place(face_z + p * inner, inner, source, skip + size * (inner + cells) + i * inner)
    mom_ref[...] = WEIGHT * jnp.transpose(sum_ref[...], (1, 0))[:COLS]


def renew_kernel(
    scal_ref, bound_ref, x_ref, cell_ref, in_ref, edge_ref, mom_ref, peer_ref, tot_ref, kind_ref,
    mask_ref, table_ref,
    *refs, planes, last, unroll,
):
    if last:
        out_ref, *refs = refs
    else:
        out_ref, next_ref, up_ref, down_ref, *refs = refs
    work_ref, wide_ref, lhs_ref, keep_ref, amp_ref, acc_ref, part_ref, *refs = refs
    res_refs, flux_refs = refs[:unroll], refs[unroll:]
    minus = scal_ref[0] > 0
    cells = ROWS * ROWS
    inner = (ROWS - 2) * ROWS
    count = planes - 2
    face_y = (planes + 1) * inner
    face_z = face_y + planes * cells
    faces = face_z + planes * inner
    own = planes * cells

    t = [mom_ref[i : i + 1, :] + peer_ref[i : i + 1, :] for i in range(COLS)]
    density, velocity, temper, heat = state_of(t)
    tau = relaxation(density, temper)
    heat = [2.0 * tau * q / (2.0 * tau + HALF * PRANDTL) for q in heat]
    divide = 1.0 / (2.0 * tau + HALF)
    keep = 2.0 * tau * divide
    amplitude = (HALF * divide) * (density / (temper * jnp.sqrt(temper)))
    turned = transposed_parts(exponent_coefs(velocity, temper), [keep], wide_ref)[:faces]
    lhs_ref[0:faces, :] = turned.astype(jnp.bfloat16)
    keep_ref[...] = spread_column(turned)
    turned = transposed_parts(
        shakhov_coefs(amplitude, density, velocity, temper, heat), [], wide_ref
    )[:faces]
    lhs_ref[faces : 2 * faces, :] = turned.astype(jnp.bfloat16)

    density = tot_ref[0:1, :]
    kind = kind_ref[:, 2 * cells : 2 * cells + own]
    inlet, outlet = kind == 2, kind == 3
    moving = [
        jnp.where(outlet, UNIT * tot_ref[1 + e : 2 + e, :] / density, 0.0) for e in range(3)
    ]
    moving[0] = jnp.where(inlet, bound_ref[1], moving[0])
    dense = jnp.where(inlet, bound_ref[0], jnp.where(outlet, bound_ref[3], density))
    warm = jnp.where(inlet, bound_ref[2], jnp.where(outlet, bound_ref[4], bound_ref[5]))
    amplitude = dense / (warm * jnp.sqrt(warm))
    turned = transposed_parts(exponent_coefs(moving, warm), [amplitude], work_ref)
    lhs_ref[2 * faces : 2 * faces + own, :] = turned.astype(jnp.bfloat16)
    amp_ref[...] = spread_column(turned)
    acc_ref[...] = jnp.zeros_like(acc_ref)

    along_y, along_z = lane_speeds((ROWS, TILE))
    hy = DT * along_y
    hz = DT * along_z

    def along_x_source(plane):
        if plane in (-1, planes):
            return edge_ref, 0
        if plane in (0, planes - 1):
            return edge_ref, inner if plane == 0 else 2 * inner
        return in_ref, (plane - 1) * inner

    def face_rows(r, lanes):
        rows = 2 * ROWS

        def load(ref, at):
            return ref[at : at + rows, lanes]

        if r < face_y:
            w, rest = divmod(r, inner)
            ref, at = along_x_source(w)
            other, there = along_x_source(w - 1)
            return jnp.where(minus, load(ref, at + rest), load(other, there + rest))
        size, start = (cells, face_y) if r < face_z else (inner, face_z)
        p, rest = divmod(r - start, size)
        outer = p in (0, planes - 1)
        i = (0 if p == 0 else 1) if outer else p - 1
        many, skip = (2, inner) if outer else (count, 0)
        before = skip + many * (inner if r < face_z else inner + cells)
        return load(edge_ref if outer else in_ref, before + i * size + rest)

    @pl.loop(0, x_ref.shape[1] // (TILE * unroll))
    def _(m):
        tables = []
        for k, res_ref in enumerate(res_refs):
            n = m * unroll + k
            table = table_ref[:, tile_lanes(scal_ref[1] + n)]
            tables.append(table)
            res_ref[...] = dot_nn(lhs_ref[...], table)
        for k, (res_ref, flux_ref) in enumerate(zip(res_refs, flux_refs)):
            n = m * unroll + k
            lanes = tile_lanes(n)
            digit = scal_ref[1] + n
            hx = (2 * digit + 1 - NODES).astype(jnp.float32) * (UNIT * DT)
            for r in range(0, faces, 16):
                rows = slice(r, r + 16)
                poly = res_ref[faces + r : faces + r + 16, :]
                flux_ref[rows, :] = (
                    twice(keep_ref[rows, :]) * face_rows(r, lanes) + jnp.exp2(res_ref[rows, :]) * poly
                )
            for p in range(planes):
                done = []
                for y in range(ROWS):
                    at = p * cells + y * ROWS
                    rows = slice(at, at + ROWS)
                    value = twice(amp_ref[rows, :]) * jnp.exp2(
                        res_ref[2 * faces + at : 2 * faces + at + ROWS, :]
                    )
                    if 0 < y < ROWS - 1:
                        ax = p * inner + (y - 1) * ROWS
                        ay = face_y + at
                        az = face_z + ax
                        along = (
                            flux_ref[ax + inner : ax + inner + ROWS, :]
                            - flux_ref[ax : ax + ROWS, :]
                        )
                        across = (
                            flux_ref[ay + ROWS : ay + 2 * ROWS, :] - flux_ref[ay : ay + ROWS, :]
                        )
                        low = flux_ref[az : az + ROWS, :]
                        rise = pltpu.roll(low, ROWS - 1, 0) - low
                        plus = (4.0 / 3.0) * cell_ref[rows, lanes] - (1.0 / 3.0) * x_ref[rows, lanes]
                        fresh = plus - (hx * along + hy * across + hz * rise)
                        at += 2 * cells
                        mask = twice(mask_ref[at : at + ROWS, :]) > 0.0
                        value = jnp.where(mask, fresh, value)
                    done.append(value)
                    if y % 2:
                        both = jnp.concatenate(done, axis=0)
                        rows = slice(p * cells + (y - 1) * ROWS, p * cells + (y + 1) * ROWS)
                        out_ref[rows, lanes] = both
                        if not last:
                            high, low = split(both)
                            first = 2 * TILE * k
                            part_ref[rows, first : first + TILE] = high
                            part_ref[rows, first + TILE : first + 2 * TILE] = low
                        done = []
        if not last:
            acc_ref[...] += dot_nt(part_ref[...], stacked_tables(tables))
            for k in range(unroll):
                add_sends(scal_ref, out_ref, up_ref, down_ref, tile_lanes(m * unroll + k))

    if not last:
        next_ref[...] = WEIGHT * jnp.transpose(acc_ref[...], (1, 0))[:COLS]


def on_device(dist, cell_type, boundary, *, spaces, vels):
    planes, across, height, local = dist.shape
    cells = across * height
    own = planes * cells
    inner = cells - 2 * height
    faces = (planes + 1) * inner + planes * cells + planes * inner
    padded = -(-faces // 128) * 128
    extended = own + 4 * cells
    ghosts = cells + 2 * inner
    faces_in = (planes - 2) * (2 * inner + cells)
    faces_edge = inner + 2 * (2 * inner + cells)
    tiles = local // TILE
    unroll = unroll_of(tiles)
    space, vel = lax.axis_index("space"), lax.axis_index("vel")
    neg = (vel < vels // 2).astype(jnp.int32)
    scal = jnp.stack(
        [
            neg,
            vel * tiles,
            jnp.where(neg == 1, 1, planes - 2),
            jnp.where(neg == 1, 0, planes - 1),
            (space > 0).astype(jnp.int32),
            (space < spaces - 1).astype(jnp.int32),
            jnp.where(neg == 1, planes - 1, 0),
        ]
    ).astype(jnp.int32)
    table = node_table()
    kinds = jnp.pad(cell_type, ((2, 2), (0, 0), (0, 0)))
    kinds = lax.dynamic_slice_in_dim(kinds, space * planes, planes + 4, 0).reshape(1, extended)

    smem = pl.BlockSpec(memory_space=pltpu.SMEM)
    vmem = pl.BlockSpec(memory_space=pltpu.VMEM)
    f32, bf16 = jnp.float32, jnp.bfloat16
    shape = lambda *dims: jax.ShapeDtypeStruct(dims, f32)
    scratch = lambda *dims: pltpu.VMEM(dims, f32)
    packed = lambda *dims: pltpu.VMEM(dims, bf16)
    params = pltpu.CompilerParams(vmem_limit_bytes=VMEM_LIMIT)
    cost = lambda us: pl.CostEstimate(
        flops=int(us * 1e9), bytes_accessed=1 << 20, transcendentals=0
    )
    short = -(-((across - 2) * (height - 2) + 2) // ROWS) * ROWS
    sends = [shape(short + cells, local), shape(short, local)]

    sender = pl.pallas_call(
        sends_kernel,
        in_specs=[smem, vmem],
        out_specs=[vmem] * 2,
        out_shape=sends,
        compiler_params=params,
        cost_estimate=cost(1),
        name="sends",
    )
    moments = pl.pallas_call(
        moments_kernel,
        in_specs=[smem] + [vmem] * 3,
        out_specs=[vmem] * 2,
        out_shape=[shape(COLS, own), shape(extended, HALFTILE)],
        scratch_shapes=[scratch(own, KEYS), scratch(KEYS, extended)],
        compiler_params=params,
        cost_estimate=cost(2),
        name="moments",
    )
    inside = pl.pallas_call(
        functools.partial(inner_kernel, planes=planes),
        in_specs=[smem] + [vmem] * 4,
        out_specs=[vmem] * 3,
        out_shape=[shape(own, local), shape(faces_in, local), shape(faces_in, KEYS)],
        scratch_shapes=[
            scratch(KEYS, own),
            packed(2 * own, KEYS),
            scratch(own, HALFTILE),
            packed(faces_in, 2 * TILE * unroll),
        ]
        + [scratch(2 * own, TILE)] * unroll,
        compiler_params=params,
        cost_estimate=cost(6),
        name="facesin",
    )
    outside = pl.pallas_call(
        functools.partial(outer_kernel, planes=planes),
        in_specs=[smem] + [vmem] * 9,
        out_specs=[vmem] * 2,
        out_shape=[shape(faces_edge, local), shape(COLS, padded)],
        scratch_shapes=[
            scratch(COLS, 4 * cells),
            scratch(KEYS, 4 * cells),
            scratch(4 * cells, KEYS),
            packed(2 * ghosts, KEYS),
            scratch(ghosts, HALFTILE),
            scratch(ghosts, TILE * unroll),
            packed(faces_edge, 2 * TILE * unroll),
            scratch(faces_edge, KEYS),
            scratch(padded, KEYS),
        ]
        + [scratch(2 * ghosts, TILE)] * unroll,
        compiler_params=params,
        cost_estimate=cost(6),
        name="faceb",
    )

    def renew(last):
        return pl.pallas_call(
            functools.partial(renew_kernel, planes=planes, last=last, unroll=unroll),
            in_specs=[smem, smem] + [vmem] * 10,
            out_specs=[vmem] * (1 if last else 4),
            out_shape=[shape(own, local)] + ([] if last else [shape(COLS, own)] + sends),
            scratch_shapes=[
                scratch(KEYS, own),
                scratch(KEYS, padded),
                packed(2 * faces + own, KEYS),
                scratch(faces, HALFTILE),
                scratch(own, HALFTILE),
                scratch(own, KEYS),
                packed(own, 2 * TILE * unroll),
            ]
            + [scratch(2 * faces + own, TILE)] * unroll
            + [scratch(faces, TILE)] * unroll,
            compiler_params=params,
            cost_estimate=cost(6),
            name="renew",
        )

    upwind, downwind = [], []
    for s in range(spaces - 1):
        for v in range(vels):
            ahead = (s * vels + v, (s + 1) * vels + v)
            back = (ahead[1], ahead[0])
            upwind.append(back if v < vels // 2 else ahead)
            downwind.append(ahead if v < vels // 2 else back)
    rising = [(s, s + 1) for s in range(spaces - 1)]
    falling = [(s + 1, s) for s in range(spaces - 1)]
    both = ("space", "vel")

    def others(part):
        if vels == 2:
            return lax.ppermute(part, "vel", [(0, 1), (1, 0)])
        return lax.psum(part, "vel") - part

    x = dist.reshape(own, local)
    up, down = sender(scal, x)
    part, mask = moments(scal, x, kinds, table)
    for turn in range(STEPS):
        last = turn == STEPS - 1
        upw = lax.ppermute(up, both, upwind)
        dn = lax.ppermute(down, both, downwind)
        totals = part + others(part)
        below = lax.ppermute(totals[:, own - 2 * cells :], "space", rising)
        above = lax.ppermute(totals[:, : 2 * cells], "space", falling)
        cell, face_in, sums = inside(scal, x, totals, mask, table)
        face_edge, part = outside(
            scal, cell, upw, dn, below, above, totals, mask, table, sums
        )
        out = renew(last)(
            scal, boundary, x, cell, face_in, face_edge, part, others(part), totals, kinds, mask,
            table,
        )
        if last:
            (x,) = out
        else:
            x, part, up, down = out
    return x.reshape(planes, across, height, local)


def solution(mesh):
    spaces, vels = mesh.shape["space"], mesh.shape["vel"]
    return jax.shard_map(
        functools.partial(on_device, spaces=spaces, vels=vels),
        mesh=mesh,
        in_specs=(P("space", None, None, "vel"), P(), P()),
        out_specs=P("space", None, None, "vel"),
        check_vma=False,
    )
```

```python
import functools
import math

import jax
import jax.numpy as jnp
import numpy as np
from jax import lax
from jax.experimental import pallas as pl
from jax.experimental.pallas import tpu as pltpu
from jax.sharding import PartitionSpec as P

NODES = 16
STEPS = 2
PRANDTL = 2.0 / 3.0
OMEGA = 0.81
MU_REF = 0.1
DT = 0.1
HALF = 0.05
VMAX = 5.0
SPACING = 2.0 * VMAX / NODES
UNIT = 0.5 * SPACING
WEIGHT = SPACING**3 / (2.0 * math.pi) ** 1.5
LOG2E = 1.4426950408889634
COLS = 16
TILE = NODES * NODES
ROWS = 8
HALFTILE = 128
KEYS = 64
VMEM_LIMIT = 24 * 2**20


def node_table():
    number = np.arange(NODES**3)
    digits = (number // (NODES * NODES), number // NODES % NODES, number % NODES)
    m = [2 * d + 1 - NODES for d in digits]
    n = m[0] * m[0] + m[1] * m[1] + m[2] * m[2]
    third = [c * n for c in m]
    high = [((v + 32) // 64) * 64 for v in third]
    low = [v - h for v, h in zip(third, high)]
    base = [np.ones_like(n), *m, m[0] * m[0], m[1] * m[1], m[2] * m[2]]
    base += [m[0] * m[1], m[0] * m[2], m[1] * m[2], *high, *low]
    table = np.zeros((KEYS, NODES**3), np.float32)
    for part in range(3):
        table[part * COLS : (part + 1) * COLS] = np.stack(base)
    return jnp.asarray(table, jnp.bfloat16)


def dot_nt(a, b):
    return lax.dot_general(a, b, (((1,), (1,)), ((), ())), preferred_element_type=jnp.float32)


def dot_nn(a, b):
    return lax.dot_general(a, b, (((1,), (0,)), ((), ())), preferred_element_type=jnp.float32)


def split(value):
    high = value.astype(jnp.bfloat16)
    low = (value - high.astype(jnp.float32)).astype(jnp.bfloat16)
    return high, low


def state_of(t):
    density = t[0]
    second_unit = UNIT * UNIT
    velocity = [UNIT * t[1 + e] / density for e in range(3)]
    second = (
        (second_unit * t[4], second_unit * t[7], second_unit * t[8]),
        (second_unit * t[7], second_unit * t[5], second_unit * t[9]),
        (second_unit * t[8], second_unit * t[9], second_unit * t[6]),
    )
    trace = second[0][0] + second[1][1] + second[2][2]
    speed_sq = velocity[0] * velocity[0] + velocity[1] * velocity[1] + velocity[2] * velocity[2]
    temper = (trace / density - speed_sq) / 3.0
    heat = [
        0.5
        * (
            (UNIT**3) * (t[10 + e] + t[13 + e])
            - 2.0
            * (
                second[e][0] * velocity[0]
                + second[e][1] * velocity[1]
                + second[e][2] * velocity[2]
            )
            - velocity[e] * trace
            + 2.0 * density * velocity[e] * speed_sq
        )
        for e in range(3)
    ]
    return density, velocity, temper, heat


def relaxation(density, temper):
    return MU_REF * jnp.exp(OMEGA * jnp.log(temper)) / (density * temper)


def exponent_coefs(velocity, temper):
    g = -0.5 * LOG2E / temper
    speed_sq = velocity[0] * velocity[0] + velocity[1] * velocity[1] + velocity[2] * velocity[2]
    square = g * (UNIT * UNIT)
    linear = [(-2.0 * UNIT) * g * velocity[e] for e in range(3)]
    return [g * speed_sq, *linear, square, square, square]


def shakhov_coefs(amplitude, density, velocity, temper, heat):
    factor = (1.0 - PRANDTL) / (5.0 * density * temper * temper)
    af = amplitude * factor
    inverse = 1.0 / temper
    along = velocity[0] * heat[0] + velocity[1] * heat[1] + velocity[2] * heat[2]
    speed_sq = velocity[0] * velocity[0] + velocity[1] * velocity[1] + velocity[2] * velocity[2]
    a2 = (UNIT * UNIT) * inverse
    b = [(-2.0 * UNIT) * velocity[e] * inverse for e in range(3)]
    c = speed_sq * inverse - 5.0
    kq = [UNIT * heat[e] for e in range(3)]
    cubic = [af * (kq[e] * a2) for e in range(3)]
    return [
        amplitude - af * (along * c),
        *[af * (kq[e] * c - along * b[e]) for e in range(3)],
        *[af * (kq[e] * b[e] - along * a2) for e in range(3)],
        af * (kq[0] * b[1] + kq[1] * b[0]),
        af * (kq[0] * b[2] + kq[2] * b[0]),
        af * (kq[1] * b[2] + kq[2] * b[1]),
        *cubic,
        *cubic,
    ]


def transposed_parts(coefs, extras, work):
    count = work.shape[1]
    work[0:COLS, :] = jnp.zeros((COLS, count), jnp.float32)
    work[3 * COLS :, :] = jnp.zeros((KEYS - 3 * COLS, count), jnp.float32)
    for row, value in enumerate(coefs):
        work[row : row + 1, :] = value
    for row, value in enumerate(extras):
        work[3 * COLS + row : 3 * COLS + row + 1, :] = value
    value = work[0:COLS, :]
    high = value.astype(jnp.bfloat16).astype(jnp.float32)
    rest = value - high
    middle = rest.astype(jnp.bfloat16).astype(jnp.float32)
    work[0:COLS, :] = high
    work[COLS : 2 * COLS, :] = middle
    work[2 * COLS : 3 * COLS, :] = rest - middle
    return jnp.transpose(work[...], (1, 0))


def spread_column(matrix, extra=0):
    at = 3 * COLS + extra
    return jnp.broadcast_to(matrix[:, at : at + 1], (matrix.shape[0], HALFTILE))


def tile_lanes(n):
    return pl.ds(pl.multiple_of(n * TILE, TILE), TILE)


def twice(value):
    return jnp.concatenate([value, value], axis=1)


def lane_speeds(shape):
    lane = lax.broadcasted_iota(jnp.int32, shape, 1)
    along_y = (2 * (lane // NODES) + 1 - NODES).astype(jnp.float32) * UNIT
    along_z = (2 * (lane % NODES) + 1 - NODES).astype(jnp.float32) * UNIT
    return along_y, along_z


def add_sends(scal_ref, x_ref, up_ref, down_ref, lanes):
    cells = ROWS * ROWS
    short = down_ref.shape[0]

    def pack(plane, ref):
        ref[short - ROWS : short, lanes] = jnp.zeros((ROWS, TILE), jnp.float32)
        for y in range(1, ROWS - 1):
            column = x_ref[pl.ds(pl.multiple_of(plane * cells + y * ROWS, ROWS), ROWS), lanes]
            first = (y - 1) * (ROWS - 2)
            if y == 1:
                ref[0:ROWS, lanes] = column
            else:
                ref[first + 1 : first + ROWS - 1, lanes] = column[1 : ROWS - 1]

    pack(scal_ref[2], up_ref)
    near = pl.multiple_of(scal_ref[3] * cells, ROWS)
    up_ref[short:, lanes] = x_ref[pl.ds(near, cells), lanes]
    pack(scal_ref[6], down_ref)


def sends_kernel(scal_ref, x_ref, up_ref, down_ref):
    for n in range(x_ref.shape[1] // TILE):
        add_sends(scal_ref, x_ref, up_ref, down_ref, slice(n * TILE, (n + 1) * TILE))


def unroll_of(tiles):
    return 8 if tiles % 8 == 0 else 4 if tiles % 4 == 0 else 2 if tiles % 2 == 0 else 1


def moments_kernel(
    scal_ref, x_ref, kind_ref, table_ref, out_ref, mask_ref, acc_ref, work_ref
):
    acc_ref[...] = jnp.zeros_like(acc_ref)
    for n in range(x_ref.shape[1] // TILE):
        high, low = split(x_ref[:, n * TILE : (n + 1) * TILE])
        table = table_ref[:, tile_lanes(scal_ref[1] + n)]
        acc_ref[...] += dot_nt(high, table) + dot_nt(low, table)

    out_ref[...] = WEIGHT * jnp.transpose(acc_ref[...], (1, 0))[:COLS]
    fluid = (kind_ref[...] == 1).astype(jnp.float32)
    mask_ref[...] = spread_column(transposed_parts([], [fluid], work_ref))


def cell_coefs(t):
    density, velocity, temper, heat = state_of(t)
    tau = relaxation(density, temper)
    heat = [q / (1.0 + DT * PRANDTL / (2.0 * tau)) for q in heat]
    divide = 1.0 / (2.0 * tau + DT)
    alpha = (2.0 * tau - HALF) * divide
    beta = (3.0 * HALF) * divide
    amplitude = beta * (density / (temper * jnp.sqrt(temper)))
    poly = shakhov_coefs(amplitude, density, velocity, temper, heat)
    return exponent_coefs(velocity, temper), poly, alpha


def middle(a, b):
    return jnp.maximum(jnp.minimum(a, b), jnp.minimum(jnp.maximum(a, b), 0.0))


class Lanes:
    def __init__(self):
        along_y, along_z = lane_speeds((ROWS, TILE))
        lane = lax.broadcasted_iota(jnp.int32, (ROWS, TILE), 1)
        self.z_minus = (lane % NODES) < NODES // 2
        self.ky = HALF * along_y
        self.kz = HALF * along_z
        self.hy = jnp.where(lane < HALFTILE, -0.5, 0.5)
        self.hz = jnp.where(self.z_minus, -0.5, 0.5)


def put_faces(face_ref, part_ref, lanes, first, row, pair):
    both = jnp.concatenate(pair, axis=0)
    high, low = split(both)
    rows = slice(row, row + 2 * ROWS)
    face_ref[rows, lanes] = both
    part_ref[rows, first : first + TILE] = high
    part_ref[rows, first + TILE : first + 2 * TILE] = low


def plane_faces(col, ahead, behind, mask_of, kx, hx, node, put, rows_x, rows_y, rows_z):
    values = {0: col(0), 1: col(1)}
    diff = values[1] - values[0]
    own = rows_y is not None
    fx, fy, fz = {}, {0: values[0]}, {}
    for y in range(1, ROWS - 1):
        here = values[y]
        values[y + 1] = col(y + 1)
        back, diff = diff, values[y + 1] - here
        mask = mask_of(y)
        slope_y = middle(diff, back) * mask
        slope_x = mask * middle(ahead(y) - here, here - behind(y))
        step = here - pltpu.roll(here, 1, 0)
        slope_z = middle(pltpu.roll(step, ROWS - 1, 0), step) * mask
        centre = here - (kx * slope_x + node.ky * slope_y + node.kz * slope_z)
        fx[y] = centre + hx * slope_x
        if own:
            fy[y] = centre + node.hy * slope_y
            side = centre + node.hz * slope_z
            fz[y] = jnp.where(node.z_minus, side, pltpu.roll(side, 1, 0))
    for i in range((ROWS - 2) // 2):
        put(rows_x + 16 * i, [fx[1 + 2 * i], fx[2 + 2 * i]])
    if own:
        fy[ROWS - 1] = values[ROWS - 1]
        gy = [fy[0]]
        for j in range(1, ROWS):
            gy.append(jnp.concatenate([fy[j][:, :HALFTILE], fy[j - 1][:, HALFTILE:]], axis=1))
        for i in range(ROWS // 2):
            put(rows_y + 16 * i, [gy[2 * i], gy[2 * i + 1]])
        for i in range((ROWS - 2) // 2):
            put(rows_z + 16 * i, [fz[1 + 2 * i], fz[2 + 2 * i]])


def x_factors(scal_ref, n):
    along_x = (2 * (scal_ref[1] + n) + 1 - NODES).astype(jnp.float32) * UNIT
    return HALF * along_x, jnp.where(along_x > 0, 0.5, -0.5)


def stacked_tables(tables):
    return jnp.concatenate([t for t in tables for _ in range(2)], axis=1)


def inner_kernel(
    scal_ref, x_ref, tot_ref, mask_ref, table_ref,
    cell_ref, face_ref, acc_ref,
    work_ref, lhs_ref, alpha_ref, part_ref, *res_refs,
    planes,
):
    cells = ROWS * ROWS
    inner = (ROWS - 2) * ROWS
    own = planes * cells
    count = planes - 2
    unroll = len(res_refs)
    exponent, poly, alpha = cell_coefs([tot_ref[i : i + 1, :] for i in range(COLS)])
    turned = transposed_parts(exponent, [alpha], work_ref)
    lhs_ref[0:own, :] = turned.astype(jnp.bfloat16)
    alpha_ref[...] = spread_column(turned)
    lhs_ref[own : 2 * own, :] = transposed_parts(poly, [], work_ref).astype(jnp.bfloat16)
    acc_ref[...] = jnp.zeros_like(acc_ref)
    node = Lanes()

    @pl.loop(0, x_ref.shape[1] // (TILE * unroll))
    def _(m):
        tables = []
        for k, res_ref in enumerate(res_refs):
            n = m * unroll + k
            lanes = tile_lanes(n)
            table = table_ref[:, tile_lanes(scal_ref[1] + n)]
            tables.append(table)
            res_ref[...] = dot_nn(lhs_ref[...], table)
            lanes = tile_lanes(n)
            kx, hx = x_factors(scal_ref, n)
            for r in range(0, own, 16):
                rows = slice(r, r + 16)
                cell_ref[rows, lanes] = twice(alpha_ref[rows, :]) * x_ref[rows, lanes] + jnp.exp2(
                    res_ref[rows, :]
                ) * res_ref[own + r : own + r + 16, :]
            put = functools.partial(put_faces, face_ref, part_ref, lanes, 2 * TILE * k)
            for i in range(count):
                base = (i + 1) * cells

                def col(y, base=base):
                    return cell_ref[base + y * ROWS : base + (y + 1) * ROWS, lanes]

                def mask_of(y, base=base):
                    at = 2 * cells + base + y * ROWS
                    return twice(mask_ref[at : at + ROWS, :])

                plane_faces(
                    col,
                    lambda y, base=base: col(y, base + cells),
                    lambda y, base=base: col(y, base - cells),
                    mask_of, kx, hx, node, put,
                    i * inner, count * inner + i * cells, count * (inner + cells) + i * inner,
                )
        acc_ref[...] += dot_nt(part_ref[...], stacked_tables(tables))


def outer_kernel(
    scal_ref, cell_ref, upw_ref, dn_ref, below_ref, above_ref, tot_ref, mask_ref, table_ref,
    inacc_ref,
    face_ref, mom_ref,
    ext_ref, work_ref, full_ref, lhs_ref, alpha_ref, slab_ref, part_ref, acc_ref, sum_ref,
    *res_refs, planes,
):
    neg = scal_ref[0]
    cells = ROWS * ROWS
    inner = (ROWS - 2) * ROWS
    own = planes * cells
    count = planes - 2
    ghosts = cells + 2 * inner
    unroll = len(res_refs)

    ext_ref[:, : 2 * cells] = jnp.where(scal_ref[4] > 0, below_ref[...], tot_ref[:, : 2 * cells])
    ext_ref[:, 2 * cells :] = jnp.where(
        scal_ref[5] > 0, above_ref[...], tot_ref[:, own - 2 * cells :]
    )
    exponent, poly, alpha = cell_coefs([ext_ref[i : i + 1, :] for i in range(COLS)])
    near = pl.ds(pl.multiple_of((1 + neg) * cells, ROWS), cells)
    far = pl.ds(pl.multiple_of(3 * neg * cells + ROWS, ROWS), inner)
    down = pl.ds(pl.multiple_of((2 - neg) * cells + ROWS, ROWS), inner)

    def gather():
        return jnp.concatenate([full_ref[far, :], full_ref[near, :], full_ref[down, :]], axis=0)

    full_ref[...] = transposed_parts(exponent, [alpha], work_ref)
    turned = gather()
    lhs_ref[0:ghosts, :] = turned.astype(jnp.bfloat16)
    alpha_ref[...] = spread_column(turned)
    full_ref[...] = transposed_parts(poly, [], work_ref)
    lhs_ref[ghosts : 2 * ghosts, :] = gather().astype(jnp.bfloat16)
    acc_ref[...] = jnp.zeros_like(acc_ref)
    node = Lanes()
    minus = neg > 0
    near_mask = pl.multiple_of((1 + (planes + 1) * neg) * cells, ROWS)

    @pl.loop(0, cell_ref.shape[1] // (TILE * unroll))
    def _(m):
        tables = []
        for k, res_ref in enumerate(res_refs):
            n = m * unroll + k
            table = table_ref[:, tile_lanes(scal_ref[1] + n)]
            tables.append(table)
            res_ref[...] = dot_nn(lhs_ref[...], table)
            lanes = tile_lanes(n)
            kx, hx = x_factors(scal_ref, n)
            for r in range(0, ghosts, 16):
                rows = slice(r, r + 16)
                short = dn_ref.shape[0]
                if inner <= r < inner + cells:
                    f = upw_ref[short + r - inner : short + r - inner + 16, lanes]
                else:
                    ref, y = (upw_ref, r // ROWS) if r < inner else (dn_ref, (r - inner - cells) // ROWS)
                    first = [(y + i) * (ROWS - 2) for i in range(2)]
                    f = jnp.concatenate([ref[a : a + ROWS, lanes] for a in first], axis=0)
                slab_ref[rows, k * TILE : (k + 1) * TILE] = twice(alpha_ref[rows, :]) * f + jnp.exp2(
                    res_ref[rows, :]
                ) * res_ref[ghosts + r : ghosts + r + 16, :]
            put = functools.partial(put_faces, face_ref, part_ref, lanes, 2 * TILE * k)

            def ghost(first, y):
                at = first + y * ROWS
                return slab_ref[at : at + ROWS, k * TILE : (k + 1) * TILE]

            far_at = functools.partial(ghost, -ROWS)
            near_at = functools.partial(ghost, inner)
            down_at = functools.partial(ghost, inner + cells - ROWS)

            def cell(plane, y):
                at = plane * cells + y * ROWS
                return cell_ref[at : at + ROWS, lanes]

            def cell_mask(plane, y):
                at = (2 + plane) * cells + y * ROWS
                return twice(mask_ref[at : at + ROWS, :])

            def ghost_mask(y):
                at = pl.multiple_of(near_mask + y * ROWS, ROWS)
                return twice(mask_ref[pl.ds(at, ROWS), :])

            end = planes - 1
            plane_faces(
                near_at,
                lambda y: jnp.where(minus, cell(end, y), cell(0, y)),
                far_at,
                ghost_mask, jnp.abs(kx), 0.5, node, put, 0, None, None,
            )
            plane_faces(
                functools.partial(cell, 0),
                functools.partial(cell, 1),
                lambda y: jnp.where(minus, down_at(y), near_at(y)),
                functools.partial(cell_mask, 0), kx, hx, node, put,
                inner, 3 * inner, 3 * inner + 2 * cells,
            )
            plane_faces(
                functools.partial(cell, end),
                lambda y: jnp.where(minus, near_at(y), down_at(y)),
                functools.partial(cell, end - 1),
                functools.partial(cell_mask, end), kx, hx, node, put,
                2 * inner, 3 * inner + cells, 4 * inner + 2 * cells,
            )
        acc_ref[...] += dot_nt(part_ref[...], stacked_tables(tables))

    face_y = (planes + 1) * inner
    face_z = face_y + planes * cells
    used = face_z + planes * inner
    if sum_ref.shape[0] > used:
        sum_ref[used:, :] = jnp.zeros((sum_ref.shape[0] - used, KEYS), jnp.float32)

    def place(row, size, source, at):
        sum_ref[pl.ds(pl.multiple_of(row, ROWS), size), :] = source[at : at + size, :]

    place(planes * neg * inner, inner, acc_ref, 0)
    for p in range(planes):
        outer = p in (0, planes - 1)
        source = acc_ref if outer else inacc_ref
        i = (0 if p == 0 else 1) if outer else p - 1
        size = 2 if outer else count
        skip = inner if outer else 0
        place((p + 1 - neg) * inner, inner, source, skip + i * inner)
        place(face_y + p * cells, cells, source, skip + size * inner + i * cells)
        place(face_z + p * inner, inner, source, skip + size * (inner + cells) + i * inner)
    mom_ref[...] = WEIGHT * jnp.transpose(sum_ref[...], (1, 0))[:COLS]


def renew_kernel(
    scal_ref, bound_ref, x_ref, cell_ref, in_ref, edge_ref, mom_ref, peer_ref, tot_ref, kind_ref,
    mask_ref, table_ref,
    *refs, planes, last, unroll,
):
    if last:
        out_ref, *refs = refs
    else:
        out_ref, next_ref, up_ref, down_ref, *refs = refs
    work_ref, wide_ref, lhs_ref, keep_ref, amp_ref, acc_ref, part_ref, *refs = refs
    res_refs, flux_refs = refs[:unroll], refs[unroll:]
    minus = scal_ref[0] > 0
    cells = ROWS * ROWS
    inner = (ROWS - 2) * ROWS
    count = planes - 2
    face_y = (planes + 1) * inner
    face_z = face_y + planes * cells
    faces = face_z + planes * inner
    own = planes * cells

    t = [mom_ref[i : i + 1, :] + peer_ref[i : i + 1, :] for i in range(COLS)]
    density, velocity, temper, heat = state_of(t)
    tau = relaxation(density, temper)
    heat = [2.0 * tau * q / (2.0 * tau + HALF * PRANDTL) for q in heat]
    divide = 1.0 / (2.0 * tau + HALF)
    keep = 2.0 * tau * divide
    amplitude = (HALF * divide) * (density / (temper * jnp.sqrt(temper)))
    turned = transposed_parts(exponent_coefs(velocity, temper), [keep], wide_ref)[:faces]
    lhs_ref[0:faces, :] = turned.astype(jnp.bfloat16)
    keep_ref[...] = spread_column(turned)
    turned = transposed_parts(
        shakhov_coefs(amplitude, density, velocity, temper, heat), [], wide_ref
    )[:faces]
    lhs_ref[faces : 2 * faces, :] = turned.astype(jnp.bfloat16)

    density = tot_ref[0:1, :]
    kind = kind_ref[:, 2 * cells : 2 * cells + own]
    inlet, outlet = kind == 2, kind == 3
    moving = [
        jnp.where(outlet, UNIT * tot_ref[1 + e : 2 + e, :] / density, 0.0) for e in range(3)
    ]
    moving[0] = jnp.where(inlet, bound_ref[1], moving[0])
    dense = jnp.where(inlet, bound_ref[0], jnp.where(outlet, bound_ref[3], density))
    warm = jnp.where(inlet, bound_ref[2], jnp.where(outlet, bound_ref[4], bound_ref[5]))
    amplitude = dense / (warm * jnp.sqrt(warm))
    turned = transposed_parts(exponent_coefs(moving, warm), [amplitude], work_ref)
    lhs_ref[2 * faces : 2 * faces + own, :] = turned.astype(jnp.bfloat16)
    amp_ref[...] = spread_column(turned)
    acc_ref[...] = jnp.zeros_like(acc_ref)

    along_y, along_z = lane_speeds((ROWS, TILE))
    hy = DT * along_y
    hz = DT * along_z

    def along_x_source(plane):
        if plane in (-1, planes):
            return edge_ref, 0
        if plane in (0, planes - 1):
            return edge_ref, inner if plane == 0 else 2 * inner
        return in_ref, (plane - 1) * inner

    def face_rows(r, lanes):
        rows = 2 * ROWS

        def load(ref, at):
            return ref[at : at + rows, lanes]

        if r < face_y:
            w, rest = divmod(r, inner)
            ref, at = along_x_source(w)
            other, there = along_x_source(w - 1)
            return jnp.where(minus, load(ref, at + rest), load(other, there + rest))
        size, start = (cells, face_y) if r < face_z else (inner, face_z)
        p, rest = divmod(r - start, size)
        outer = p in (0, planes - 1)
        i = (0 if p == 0 else 1) if outer else p - 1
        many, skip = (2, inner) if outer else (count, 0)
        before = skip + many * (inner if r < face_z else inner + cells)
        return load(edge_ref if outer else in_ref, before + i * size + rest)

    @pl.loop(0, x_ref.shape[1] // (TILE * unroll))
    def _(m):
        tables = []
        for k, res_ref in enumerate(res_refs):
            n = m * unroll + k
            table = table_ref[:, tile_lanes(scal_ref[1] + n)]
            tables.append(table)
            res_ref[...] = dot_nn(lhs_ref[...], table)
            flux_ref = flux_refs[k]
            lanes = tile_lanes(n)
            digit = scal_ref[1] + n
            hx = (2 * digit + 1 - NODES).astype(jnp.float32) * (UNIT * DT)
            for r in range(0, faces, 16):
                rows = slice(r, r + 16)
                poly = res_ref[faces + r : faces + r + 16, :]
                flux_ref[rows, :] = (
                    twice(keep_ref[rows, :]) * face_rows(r, lanes) + jnp.exp2(res_ref[rows, :]) * poly
                )
            for p in range(planes):
                done = []
                for y in range(ROWS):
                    at = p * cells + y * ROWS
                    rows = slice(at, at + ROWS)
                    value = twice(amp_ref[rows, :]) * jnp.exp2(
                        res_ref[2 * faces + at : 2 * faces + at + ROWS, :]
                    )
                    if 0 < y < ROWS - 1:
                        ax = p * inner + (y - 1) * ROWS
                        ay = face_y + at
                        az = face_z + ax
                        along = (
                            flux_ref[ax + inner : ax + inner + ROWS, :]
                            - flux_ref[ax : ax + ROWS, :]
                        )
                        across = (
                            flux_ref[ay + ROWS : ay + 2 * ROWS, :] - flux_ref[ay : ay + ROWS, :]
                        )
                        low = flux_ref[az : az + ROWS, :]
                        rise = pltpu.roll(low, ROWS - 1, 0) - low
                        plus = (4.0 / 3.0) * cell_ref[rows, lanes] - (1.0 / 3.0) * x_ref[rows, lanes]
                        fresh = plus - (hx * along + hy * across + hz * rise)
                        at += 2 * cells
                        mask = twice(mask_ref[at : at + ROWS, :]) > 0.0
                        value = jnp.where(mask, fresh, value)
                    done.append(value)
                    if y % 2:
                        both = jnp.concatenate(done, axis=0)
                        rows = slice(p * cells + (y - 1) * ROWS, p * cells + (y + 1) * ROWS)
                        out_ref[rows, lanes] = both
                        if not last:
                            high, low = split(both)
                            first = 2 * TILE * k
                            part_ref[rows, first : first + TILE] = high
                            part_ref[rows, first + TILE : first + 2 * TILE] = low
                        done = []
        if not last:
            acc_ref[...] += dot_nt(part_ref[...], stacked_tables(tables))
            for k in range(unroll):
                add_sends(scal_ref, out_ref, up_ref, down_ref, tile_lanes(m * unroll + k))

    if not last:
        next_ref[...] = WEIGHT * jnp.transpose(acc_ref[...], (1, 0))[:COLS]


def on_device(dist, cell_type, boundary, *, spaces, vels):
    planes, across, height, local = dist.shape
    cells = across * height
    own = planes * cells
    inner = cells - 2 * height
    faces = (planes + 1) * inner + planes * cells + planes * inner
    padded = -(-faces // 128) * 128
    extended = own + 4 * cells
    ghosts = cells + 2 * inner
    faces_in = (planes - 2) * (2 * inner + cells)
    faces_edge = inner + 2 * (2 * inner + cells)
    tiles = local // TILE
    unroll = unroll_of(tiles)
    space, vel = lax.axis_index("space"), lax.axis_index("vel")
    neg = (vel < vels // 2).astype(jnp.int32)
    scal = jnp.stack(
        [
            neg,
            vel * tiles,
            jnp.where(neg == 1, 1, planes - 2),
            jnp.where(neg == 1, 0, planes - 1),
            (space > 0).astype(jnp.int32),
            (space < spaces - 1).astype(jnp.int32),
            jnp.where(neg == 1, planes - 1, 0),
        ]
    ).astype(jnp.int32)
    table = node_table()
    kinds = jnp.pad(cell_type, ((2, 2), (0, 0), (0, 0)))
    kinds = lax.dynamic_slice_in_dim(kinds, space * planes, planes + 4, 0).reshape(1, extended)

    smem = pl.BlockSpec(memory_space=pltpu.SMEM)
    vmem = pl.BlockSpec(memory_space=pltpu.VMEM)
    f32, bf16 = jnp.float32, jnp.bfloat16
    shape = lambda *dims: jax.ShapeDtypeStruct(dims, f32)
    scratch = lambda *dims: pltpu.VMEM(dims, f32)
    packed = lambda *dims: pltpu.VMEM(dims, bf16)
    params = pltpu.CompilerParams(vmem_limit_bytes=VMEM_LIMIT)
    cost = lambda us: pl.CostEstimate(
        flops=int(us * 1e9), bytes_accessed=1 << 20, transcendentals=0
    )
    short = -(-((across - 2) * (height - 2) + 2) // ROWS) * ROWS
    sends = [shape(short + cells, local), shape(short, local)]

    sender = pl.pallas_call(
        sends_kernel,
        in_specs=[smem, vmem],
        out_specs=[vmem] * 2,
        out_shape=sends,
        compiler_params=params,
        cost_estimate=cost(1),
        name="sends",
    )
    moments = pl.pallas_call(
        moments_kernel,
        in_specs=[smem] + [vmem] * 3,
        out_specs=[vmem] * 2,
        out_shape=[shape(COLS, own), shape(extended, HALFTILE)],
        scratch_shapes=[scratch(own, KEYS), scratch(KEYS, extended)],
        compiler_params=params,
        cost_estimate=cost(2),
        name="moments",
    )
    inside = pl.pallas_call(
        functools.partial(inner_kernel, planes=planes),
        in_specs=[smem] + [vmem] * 4,
        out_specs=[vmem] * 3,
        out_shape=[shape(own, local), shape(faces_in, local), shape(faces_in, KEYS)],
        scratch_shapes=[
            scratch(KEYS, own),
            packed(2 * own, KEYS),
            scratch(own, HALFTILE),
            packed(faces_in, 2 * TILE * unroll),
        ]
        + [scratch(2 * own, TILE)] * unroll,
        compiler_params=params,
        cost_estimate=cost(6),
        name="facesin",
    )
    outside = pl.pallas_call(
        functools.partial(outer_kernel, planes=planes),
        in_specs=[smem] + [vmem] * 9,
        out_specs=[vmem] * 2,
        out_shape=[shape(faces_edge, local), shape(COLS, padded)],
        scratch_shapes=[
            scratch(COLS, 4 * cells),
            scratch(KEYS, 4 * cells),
            scratch(4 * cells, KEYS),
            packed(2 * ghosts, KEYS),
            scratch(ghosts, HALFTILE),
            scratch(ghosts, TILE * unroll),
            packed(faces_edge, 2 * TILE * unroll),
            scratch(faces_edge, KEYS),
            scratch(padded, KEYS),
        ]
        + [scratch(2 * ghosts, TILE)] * unroll,
        compiler_params=params,
        cost_estimate=cost(6),
        name="faceb",
    )

    def renew(last):
        return pl.pallas_call(
            functools.partial(renew_kernel, planes=planes, last=last, unroll=unroll),
            in_specs=[smem, smem] + [vmem] * 10,
            out_specs=[vmem] * (1 if last else 4),
            out_shape=[shape(own, local)] + ([] if last else [shape(COLS, own)] + sends),
            scratch_shapes=[
                scratch(KEYS, own),
                scratch(KEYS, padded),
                packed(2 * faces + own, KEYS),
                scratch(faces, HALFTILE),
                scratch(own, HALFTILE),
                scratch(own, KEYS),
                packed(own, 2 * TILE * unroll),
            ]
            + [scratch(2 * faces + own, TILE)] * unroll
            + [scratch(faces, TILE)] * unroll,
            compiler_params=params,
            cost_estimate=cost(6),
            name="renew",
        )

    upwind, downwind = [], []
    for s in range(spaces - 1):
        for v in range(vels):
            ahead = (s * vels + v, (s + 1) * vels + v)
            back = (ahead[1], ahead[0])
            upwind.append(back if v < vels // 2 else ahead)
            downwind.append(ahead if v < vels // 2 else back)
    rising = [(s, s + 1) for s in range(spaces - 1)]
    falling = [(s + 1, s) for s in range(spaces - 1)]
    both = ("space", "vel")

    def others(part):
        if vels == 2:
            return lax.ppermute(part, "vel", [(0, 1), (1, 0)])
        return lax.psum(part, "vel") - part

    x = dist.reshape(own, local)
    up, down = sender(scal, x)
    part, mask = moments(scal, x, kinds, table)
    for turn in range(STEPS):
        last = turn == STEPS - 1
        upw = lax.ppermute(up, both, upwind)
        dn = lax.ppermute(down, both, downwind)
        totals = part + others(part)
        below = lax.ppermute(totals[:, own - 2 * cells :], "space", rising)
        above = lax.ppermute(totals[:, : 2 * cells], "space", falling)
        cell, face_in, sums = inside(scal, x, totals, mask, table)
        face_edge, part = outside(
            scal, cell, upw, dn, below, above, totals, mask, table, sums
        )
        out = renew(last)(
            scal, boundary, x, cell, face_in, face_edge, part, others(part), totals, kinds, mask,
            table,
        )
        if last:
            (x,) = out
        else:
            x, part, up, down = out
    return x.reshape(planes, across, height, local)


def solution(mesh):
    spaces, vels = mesh.shape["space"], mesh.shape["vel"]
    return jax.shard_map(
        functools.partial(on_device, spaces=spaces, vels=vels),
        mesh=mesh,
        in_specs=(P("space", None, None, "vel"), P(), P()),
        out_specs=P("space", None, None, "vel"),
        check_vma=False,
    )
```
